128 devices in a mesh: flow: 32 (over y, x, core), chem: 4 (over z).
Axes of the slice: x: 4, y: 4, z: 4, core: 2. Of those that a mesh axis runs over, the one named last changes fastest.
Arguments:
- component_levels: float32 [2048, 111, 512], P('flow', None, 'chem'), may hold values from 0.1 to 2
- thermal_field: float32 [2048, 512], P('flow', 'chem'), may hold values from 0.5 to 2.7
- reciprocal_pair_diffusivity: float32 [111, 111], replicated, may hold values from 0.005 to 0.02
- log_arrhenius_factor: float32 [784], replicated, may hold values from -1 to 6
- kinetic_exponents: float32 [784, 111], replicated, may hold values from 0 to 0.05
- arrhenius_energies: float32 [784], replicated, may hold values from 0.5 to 4
- molar_change_matrix: float32 [111, 784], replicated, may hold values from -0.21875 to 0.21875
- cooling_by_component: float32 [111], replicated, may hold values from -1 to 1
- burning_flags: int32 [2048, 4], P('flow', 'chem'), may hold values from 0 to 1, as said below
Outputs:
- advanced_components: float32 [2048, 111, 512], P('flow', None, 'chem')
- advanced_thermal: float32 [2048, 512], P('flow', 'chem')
The draws below stay inside these ranges and needn't reach their ends.
Inputs may be any that keep to these rules, and one draw needn't show every extreme that they name: `burning_flags`: each device's 64 rows hold at most 24 reacting blocks, and at least one device of every chem index holds exactly 24; the devices of one chem index hold exactly 256 reacting blocks together.
All inputs are finite; a program needn't handle non-finite values.
Results may differ from the reference program's by a relative error of at most 0.000058.
Values sent between devices are 32-bit elements; how exact they have to be, the bound alone decides.
No kernel may reach another device: no remote copies, remote signals or barrier semaphores. Data moves between devices by JAX's collectives and lax.ppermute only.
A program may use at most 192 MiB of HBM per device.

```python
import math
from functools import partial
import jax
import jax.numpy as jnp
from jax import lax

COMPONENTS = 111
R = 784
PATCH_POINTS = 128
CX = 64
AVG = 8
MOST = 24
LEADING_POINTS = 2048
TRAILING_POINTS = 512
N_FLOW = 32
N_CHEM = 4


def draw_thermal_field(key, part):
    noise_key = jax.random.fold_in(key, 11)
    ramp = (jnp.arange(LEADING_POINTS, dtype=jnp.float32) / max(LEADING_POINTS - 1, 1))[:, None]
    rough = jax.random.uniform(noise_key, (LEADING_POINTS, TRAILING_POINTS), jnp.float32, -0.2, 0.2)
    return 0.7 + 1.4 * ramp + rough


def column_counts(key):
    moves = 4 * N_FLOW
    keys = jax.random.split(key, 4)
    givers = jax.random.randint(keys[0], (moves,), 0, N_FLOW)
    takers = jax.random.randint(keys[1], (moves,), 0, N_FLOW)
    amounts = jax.random.randint(keys[2], (moves,), 0, MOST + 1)
    leader = jax.random.randint(keys[3], (), 0, N_FLOW)

    def shuffle(index, counts):
        giver = givers[index]
        taker = takers[index]
        amount = jnp.minimum(amounts[index], jnp.minimum(counts[giver], MOST - counts[taker]))
        amount = jnp.where(giver == taker, 0, amount)
        return counts.at[giver].add(-amount).at[taker].add(amount)
    counts = lax.fori_loop(0, moves, shuffle, jnp.full((N_FLOW,), AVG, jnp.int32))

    def gather_up(index, counts):
        amount = jnp.minimum(counts[index], MOST - counts[leader])
        amount = jnp.where(index == leader, 0, amount)
        return counts.at[index].add(-amount).at[leader].add(amount)
    return lax.fori_loop(0, N_FLOW, gather_up, counts)


def draw_burning_flags(key, part):

    def column(column_key):
        count_key, place_key = jax.random.split(column_key)
        counts = column_counts(count_key)
        orders = jax.vmap(lambda inner: jax.random.permutation(inner, CX))(jax.random.split(place_key, N_FLOW))
        return (orders < counts[:, None]).astype(jnp.int32).reshape(LEADING_POINTS)
    columns = jax.vmap(column)(jax.random.split(jax.random.fold_in(key, 29), N_CHEM))
    return columns.T


def block_scale(stream_key, dims, cuts, low, largest):
    def one(axis_at, parts):
        heights = jax.random.uniform(jax.random.fold_in(jax.random.fold_in(stream_key, 6), axis_at), (parts,), jnp.float32, low / len(cuts), largest / len(cuts))
        return jnp.repeat(jnp.exp(heights), dims[axis_at] // parts).reshape((-1,) + (1,) * (len(dims) - axis_at - 1))

    gain = one(*cuts[0])
    for cut in cuts[1:]:
        gain = gain * one(*cut)
    return gain


def gaussian(own_key, extent, spread, limit, held_as=jnp.bfloat16):
    return jnp.clip(spread * jax.random.normal(own_key, extent, jnp.float32), -limit, limit).astype(held_as)


def setup_inputs(seed: int = 0) -> dict:
    seeds = jax.random.split(jax.random.key(seed), 10)
    component_levels = jnp.clip(jnp.exp(math.log(2.0) - 2.9957323 * jax.random.uniform(seeds[0], (LEADING_POINTS, COMPONENTS, TRAILING_POINTS), jnp.float32) ** block_scale(seeds[0], (LEADING_POINTS, COMPONENTS, TRAILING_POINTS), ((0, 32), (2, 4)), -0.2, 0.2)), 0.1, 2.0)
    thermal_field = draw_thermal_field(jax.random.fold_in(seeds[9], 71), 0)
    reciprocal_pair_diffusivity = jnp.clip(jnp.exp(jax.random.uniform(seeds[2], (COMPONENTS, COMPONENTS), jnp.float32, math.log(0.005), math.log(0.02))), 0.005, 0.02)
    log_arrhenius_factor = jnp.clip(jax.random.uniform(seeds[3], (R,), jnp.float32, -1.0, 6.0), -1.0, 6.0)
    kinetic_exponents = jnp.clip(jax.random.uniform(seeds[4], (R, COMPONENTS), jnp.float32, 0.0, 0.05), 0.0, 0.05)
    arrhenius_energies = jnp.clip(jax.random.uniform(seeds[5], (R,), jnp.float32, 0.5, 4.0), 0.5, 4.0)
    molar_change_matrix = gaussian(seeds[6], (COMPONENTS, R), R ** -0.5, 0.21875, jnp.float32)
    cooling_by_component = gaussian(seeds[7], (COMPONENTS,), 0.2, 1.0, jnp.float32)
    burning_flags = draw_burning_flags(jax.random.fold_in(seeds[9], 71), 0)
    return {"component_levels": component_levels, "thermal_field": thermal_field, "reciprocal_pair_diffusivity": reciprocal_pair_diffusivity, "log_arrhenius_factor": log_arrhenius_factor, "kinetic_exponents": kinetic_exponents, "arrhenius_energies": arrhenius_energies, "molar_change_matrix": molar_change_matrix, "cooling_by_component": cooling_by_component, "burning_flags": burning_flags}


maximal_load = lax.Precision.HIGHEST
courant = 0.2
chem_step = 0.05
log_offset = 0.001
rate_ceiling = 2.0

def blend_mean(component_levels, thermal_field, reciprocal_pair_diffusivity):
    denominator = jnp.einsum('kj,xjy->xky', reciprocal_pair_diffusivity, component_levels, precision=maximal_load)
    scaled_thermal_field = thermal_field * jnp.sqrt(thermal_field)
    return scaled_thermal_field[:, None, :] / denominator

def diffuse(padded_species, padded_diffusivity, time_step):
    row_count = padded_species.shape[0] - 2
    col_count = padded_species.shape[2] - 2
    center = padded_species[1:-1, :, 1:-1]
    center_diff = padded_diffusivity[1:-1, :, 1:-1]
    flux_sum = jnp.zeros_like(center)
    for row_shift, col_shift in ((0, 1), (2, 1), (1, 0), (1, 2)):
        neighbour = padded_species[row_shift:row_shift + row_count, :, col_shift:col_shift + col_count]
        neighbour_diff = padded_diffusivity[row_shift:row_shift + row_count, :, col_shift:col_shift + col_count]
        flux_sum = flux_sum + 0.5 * (center_diff + neighbour_diff) * (neighbour - center)
    return center + time_step * flux_sum

def production(state, inverse_theta, log_arrhenius_factor, kinetic_exponents, arrhenius_energies, molar_change_matrix):
    log_conc = jnp.log(jnp.abs(state) + log_offset)
    log_rate = log_arrhenius_factor[:, None] + jnp.dot(kinetic_exponents, log_conc, precision=maximal_load) - arrhenius_energies[:, None] * inverse_theta
    reaction_rate = jnp.exp(jnp.minimum(log_rate, rate_ceiling))
    return jnp.dot(molar_change_matrix, reaction_rate, precision=maximal_load)

def combust_patches(patches, thermal_values, log_arrhenius_factor, kinetic_exponents, arrhenius_energies, molar_change_matrix, cooling_by_component):
    patch_total, species_count, patch_points = patches.shape
    beginning = patches.transpose(1, 0, 2).reshape(species_count, patch_total * patch_points)
    inverse_theta = (1.0 / thermal_values).reshape(1, patch_total * patch_points)
    rhs = partial(production, inverse_theta=inverse_theta, log_arrhenius_factor=log_arrhenius_factor, kinetic_exponents=kinetic_exponents, arrhenius_energies=arrhenius_energies, molar_change_matrix=molar_change_matrix)
    first = rhs(beginning)
    second = rhs(beginning + 0.5 * chem_step * first)
    third = rhs(beginning + 0.5 * chem_step * second)
    fourth = rhs(beginning + chem_step * third)
    concluding = beginning + chem_step / 6.0 * (first + 2.0 * second + 2.0 * third + fourth)
    thermal_result = thermal_values - jnp.dot(cooling_by_component, concluding - beginning, precision=maximal_load).reshape(patch_total, patch_points)
    return (concluding.reshape(species_count, patch_total, patch_points).transpose(1, 0, 2), thermal_result)

def reference(component_levels, thermal_field, reciprocal_pair_diffusivity, log_arrhenius_factor, kinetic_exponents, arrhenius_energies, molar_change_matrix, cooling_by_component, burning_flags):
    blended_spreading_rate = blend_mean(component_levels, thermal_field, reciprocal_pair_diffusivity)
    time_step = courant / jnp.max(blended_spreading_rate)
    edges = ((1, 1), (0, 0), (1, 1))
    diffused = diffuse(jnp.pad(component_levels, edges), jnp.pad(blended_spreading_rate, edges), time_step)
    species_count = component_levels.shape[1]
    whole_patches = diffused.reshape(LEADING_POINTS, species_count, N_CHEM, PATCH_POINTS).transpose(0, 2, 1, 3).reshape(LEADING_POINTS * N_CHEM, species_count, PATCH_POINTS)
    patchwise_thermal = thermal_field.reshape(LEADING_POINTS * N_CHEM, PATCH_POINTS)
    patch_grand_total = AVG * N_FLOW * N_CHEM
    enumerated = jnp.argsort(1 - burning_flags.reshape(-1), stable=True)[:patch_grand_total].astype(jnp.int32)

    def one_group(picked_patches):
        return combust_patches(whole_patches[picked_patches], patchwise_thermal[picked_patches], log_arrhenius_factor, kinetic_exponents, arrhenius_energies, molar_change_matrix, cooling_by_component)
    new_blocks, fresh_thermal = lax.map(one_group, enumerated.reshape(-1, AVG))
    whole_patches = whole_patches.at[enumerated].set(new_blocks.reshape(patch_grand_total, species_count, PATCH_POINTS))
    patchwise_thermal = patchwise_thermal.at[enumerated].set(fresh_thermal.reshape(patch_grand_total, PATCH_POINTS))
    advanced_components = whole_patches.reshape(LEADING_POINTS, N_CHEM, species_count, PATCH_POINTS).transpose(0, 2, 1, 3).reshape(LEADING_POINTS, species_count, TRAILING_POINTS)
    return (advanced_components, patchwise_thermal.reshape(LEADING_POINTS, TRAILING_POINTS))
```

```python
import functools

import jax
import jax.numpy as jnp
from jax import lax
from jax.experimental import pallas as pl
from jax.experimental.pallas import tpu as pltpu
from jax.sharding import Mesh
from jax.sharding import PartitionSpec as P

FLOW = ("flow_0", "flow_1", "flow_2")
FLOW_CHEM = ("flow_0", "flow_1", "flow_2", "chem")

COURANT = 0.2
CHEM_STEP = 0.05
LOG_OFFSET = 0.001
RATE_CEILING = 2.0
LOG2E = 1.4426950408889634

F32 = jnp.float32
BF16 = jnp.bfloat16
LANES = 128
GROUP = 4
CHUNK = 8


def split2(value):
    high = value.astype(BF16)
    return high, (value - high.astype(F32)).astype(BF16)


def split3(value):
    high = value.astype(BF16)
    rest = value - high.astype(F32)
    mid = rest.astype(BF16)
    return high, mid, (rest - mid.astype(F32)).astype(BF16)


def mxu(lhs, rhs):
    return jnp.dot(lhs, rhs, preferred_element_type=F32)


def mixture(cells, stacked):
    padded = cells.shape[0]
    high, low = split2(cells)
    both = mxu(stacked[...], high)
    total = both[:padded] + both[padded:] + mxu(stacked[0:padded], low)
    heat = cells[padded - 1 : padded]
    there = heat > 0.0
    scaled = heat * jnp.sqrt(heat)
    return jnp.where(there, scaled, 0.0) / jnp.where(there, total, 1.0)


def lane_index(shape):
    return lax.broadcasted_iota(jnp.int32, shape, len(shape) - 1)


def spread_kernel(
    species, reactions, x_ref, t_ref, r_ref, a_ref, k_ref, e_ref, m_ref,
    c_ref, d_ref, top_ref, bottom_ref, cols_ref, peak_ref, rs_ref, ka_ref, ms_ref,
    square, rows, tall, wide,
):
    padded = c_ref.shape[1]
    step = pl.program_id(0)

    @pl.when(step == 0)
    def _():
        square[...] = jnp.zeros_like(square)
        square[0:species, 0:species] = r_ref[...]
        square[species:padded, 0:species] = r_ref[0 : padded - species, :]
        high, low = split2(square[:, 0:padded])
        rs_ref[0:padded] = high
        rs_ref[padded : 2 * padded] = low

        tall[...] = jnp.zeros_like(tall)
        tall[:, 0:species] = k_ref[...]
        rows[...] = jnp.zeros_like(rows)
        factors = split3(a_ref[...] * LOG2E)
        energies = split3(e_ref[...] * LOG2E)
        order = [factors[0], factors[1], factors[2]] + [energies[i] for i in (0, 0, 0, 1, 1, 2)]
        for i, row in enumerate(order):
            rows[padded + i : padded + i + 1, 0:reactions] = row.astype(F32)
        for start in range(0, reactions, LANES):
            size = min(LANES, reactions - start)
            turned = rows[:, start : start + LANES].T[0:size]
            high, low = split2(tall[start : start + size, :])
            ka_ref[start : start + size, 0:LANES] = high + turned.astype(BF16)
            ka_ref[start : start + size, LANES : 2 * LANES] = low

        wide[...] = jnp.zeros_like(wide)
        wide[0:species] = m_ref[...]
        high, low = split2(wide[...])
        ms_ref[0:padded] = high
        ms_ref[padded : 2 * padded] = low
        peak_ref[...] = jnp.zeros_like(peak_ref)
        cols_ref[...] = jnp.zeros_like(cols_ref)

    flat = x_ref.reshape(species * CHUNK, LANES)
    lane = lane_index((padded, LANES))
    edges = jnp.zeros((padded, LANES), F32)
    peak = jnp.zeros((padded, LANES), F32)
    for pair in range(0, CHUNK, 2):
        for r in (pair, pair + 1):
            c_ref[r, 0:species] = flat[pl.ds(r, species, stride=CHUNK), :]
            c_ref[r, species:padded] = t_ref[r : r + 1, :]
        cells = jnp.concatenate([c_ref[pair], c_ref[pair + 1]], axis=1)
        spread = mixture(cells, rs_ref)
        d_ref[pair] = spread[:, 0:LANES]
        d_ref[pair + 1] = spread[:, LANES:]
        peak = jnp.maximum(peak, jnp.maximum(spread[:, 0:LANES], spread[:, LANES:]))
        for r in (pair, pair + 1):
            row = cells[:, (r - pair) * LANES : (r - pair + 1) * LANES]
            edges = jnp.where(lane == r, pltpu.roll(row, r, 1) if r else row, edges)
            edges = jnp.where(lane == 64 + r, pltpu.roll(row, 65 + r, 1), edges)
    moved = pltpu.roll(edges, step * CHUNK, 1)
    mine = jnp.bitwise_and(lane, 63) // CHUNK == step
    cols_ref[...] = jnp.where(mine, moved, cols_ref[...])

    @pl.when(step == 0)
    def _():
        top_ref[...] = c_ref[0]

    @pl.when(step == pl.num_programs(0) - 1)
    def _():
        bottom_ref[...] = c_ref[CHUNK - 1]

    best = jnp.maximum(peak_ref[...], jnp.max(jnp.max(peak, axis=0, keepdims=True), axis=1, keepdims=True))
    peak_ref[...] = best


def advance_kernel(
    species, reactions,
    flag_ref, peak_ref, c_ref, d_ref, up_ref, down_ref, left_ref, right_ref, cols_ref,
    t_ref, rs_ref, ka_ref, ms_ref, cool_ref,
    out_hbm, heat_ref,
    v_ref, edge_ref, outer_ref, gap_ref, order_ref, base_ref, k_ref, sum_ref, log_ref, high_ref, low_ref,
    cool_col, sems,
):
    row_count, padded, _ = c_ref.shape
    lane = lane_index((padded, LANES))

    def gather(x, found):
        order_ref[found] = x
        return found + flag_ref[x]

    live = lax.fori_loop(0, row_count, gather, jnp.int32(0))

    largest = jnp.max(peak_ref[...], axis=1, keepdims=True)
    half_step = 0.5 * (COURANT / largest)

    left = pltpu.roll(left_ref[...], 64, 1)
    right = pltpu.roll(right_ref[...], 64, 1)
    beyond = jnp.where(lane < 64, left, right)
    mine = cols_ref[...]
    spread = mixture(jnp.concatenate([mine, beyond], axis=1), rs_ref)
    edge_ref[...] = (spread[:, 0:LANES] + spread[:, LANES:]) * (beyond - mine)
    spread = mixture(jnp.concatenate([up_ref[...], down_ref[...]], axis=1), rs_ref)
    outer_ref[0] = spread[:, 0:LANES]
    outer_ref[1] = spread[:, LANES:]

    def row_flux(x, below, below_spread):
        here = c_ref[x]
        here_spread = d_ref[x]
        gap = (here_spread + below_spread) * (below - here)
        after = pltpu.roll(here, LANES - 1, 1)
        after_spread = pltpu.roll(here_spread, LANES - 1, 1)
        flux = (here_spread + after_spread) * (after - here)
        edge = edge_ref[...]
        flux = jnp.where(lane == LANES - 1, pltpu.roll(edge, 63 - x, 1), flux)
        before = jnp.where(lane == 0, -pltpu.roll(edge, LANES - x, 1), pltpu.roll(flux, 1, 1))
        v_ref[x] = here + half_step * ((flux - before) + (gap - gap_ref[...]))
        gap_ref[...] = gap

    gap_ref[...] = (d_ref[0] + outer_ref[0]) * (c_ref[0] - up_ref[...])

    @pl.loop(0, row_count - 1)
    def _(x):
        row_flux(x, c_ref[x + 1], d_ref[x + 1])
        pltpu.make_async_copy(v_ref.at[x, pl.ds(0, species)], out_hbm.at[:, x, :], sems.at[0]).start()

    row_flux(row_count - 1, down_ref[...], outer_ref[1])
    pltpu.make_async_copy(v_ref.at[row_count - 1, pl.ds(0, species)], out_hbm.at[:, row_count - 1, :], sems.at[0]).start()

    heat_ref[...] = t_ref[...]
    cool_col[...] = jnp.broadcast_to(cool_ref[...], cool_col.shape)

    def wait_rows(x, _):
        pltpu.make_async_copy(v_ref.at[0, pl.ds(0, species)], out_hbm.at[:, 0, :], sems.at[0]).wait()
        return 0

    lax.fori_loop(0, row_count, wait_rows, 0)

    log_ref[...] = jnp.zeros_like(log_ref)
    ceiling = RATE_CEILING * LOG2E

    def production(state):
        high, low = split2(jnp.log2(jnp.abs(state) + LOG_OFFSET))
        log_ref[0:padded] = high
        log_ref[LANES : LANES + padded] = high
        log_ref[2 * LANES : 2 * LANES + padded] = low
        log_ref[3 * LANES : 3 * LANES + padded] = low
        for start in range(0, reactions, 112):
            table = ka_ref[start : start + 112]
            rate = mxu(table, log_ref[0 : 2 * LANES]) + mxu(table, log_ref[2 * LANES : 4 * LANES])
            rate = jnp.exp2(jnp.minimum(rate, ceiling))
            high, low = split2(rate)
            high_ref[start : start + 112] = high
            low_ref[start : start + 112] = low
        both = mxu(ms_ref[...], high_ref[...])
        return both[0:padded] + both[padded:] + mxu(ms_ref[0:padded], low_ref[...])

    @pl.loop(0, (live + GROUP - 1) // GROUP)
    def _(group):
        places = [order_ref[jnp.minimum(group * GROUP + i, live - 1)] for i in range(GROUP)]
        for i, x in enumerate(places):
            base_ref[:, i * LANES : (i + 1) * LANES] = v_ref[x]
        heat = jnp.concatenate([t_ref[pl.ds(x, 1), :] for x in places], axis=1)
        parts = split3(-1.0 / heat)
        one = jnp.ones_like(parts[0])
        zero = jnp.zeros_like(one)
        extra = [one, one, one] + [parts[i] for i in (0, 1, 2, 0, 1, 0)] + [zero] * 7
        log_ref[padded:LANES] = jnp.concatenate(extra, axis=0)

        k_ref[...] = production(base_ref[...])
        sum_ref[...] = k_ref[...]
        k_ref[...] = production(base_ref[...] + 0.5 * CHEM_STEP * k_ref[...])
        sum_ref[...] += 2.0 * k_ref[...]
        k_ref[...] = production(base_ref[...] + 0.5 * CHEM_STEP * k_ref[...])
        sum_ref[...] += 2.0 * k_ref[...]
        total = sum_ref[...] + production(base_ref[...] + CHEM_STEP * k_ref[...])
        change = CHEM_STEP / 6.0 * total
        result = base_ref[...] + change
        moved = result - base_ref[...]
        for i, x in enumerate(places):
            lanes = slice(i * LANES, (i + 1) * LANES)
            drop = jnp.sum(cool_col[...] * moved[:, lanes], axis=0, keepdims=True)
            heat_ref[pl.ds(x, 1), :] = t_ref[pl.ds(x, 1), :] - drop

        for i, x in enumerate(places):
            @pl.when(group * GROUP + i < live)
            def _():
                v_ref[x] = result[:, i * LANES : (i + 1) * LANES]
                pltpu.make_async_copy(v_ref.at[x, pl.ds(0, species)], out_hbm.at[:, x, :], sems.at[1]).start()

    def wait_live(x, _):
        pltpu.make_async_copy(v_ref.at[0, pl.ds(0, species)], out_hbm.at[:, 0, :], sems.at[1]).wait()
        return 0

    lax.fori_loop(0, live, wait_live, 0)


def per_device(levels, heat, inverse, factor, exponents, energies, change, cooling, flags):
    row_count, species, _ = levels.shape
    reactions = factor.shape[0]
    padded = -(-species // 16) * 16
    across = -(-reactions // LANES) * LANES
    whole = pl.BlockSpec(memory_space=pltpu.VMEM)

    def fixed(*shape):
        return pl.BlockSpec(shape, lambda i: (0,) * len(shape))

    def shape(*dims, dtype=F32):
        return jax.ShapeDtypeStruct(dims, dtype)

    cells, spread, top, bottom, cols, peak, stacked, table, matrix = pl.pallas_call(
        functools.partial(spread_kernel, species, reactions),
        grid=(row_count // CHUNK,),
        in_specs=[
            pl.BlockSpec((species, CHUNK, LANES), lambda i: (0, i, 0)),
            pl.BlockSpec((CHUNK, LANES), lambda i: (i, 0)),
            fixed(species, species), fixed(1, reactions), fixed(reactions, species),
            fixed(1, reactions), fixed(species, reactions),
        ],
        out_specs=[
            pl.BlockSpec((CHUNK, padded, LANES), lambda i: (i, 0, 0)),
            pl.BlockSpec((CHUNK, padded, LANES), lambda i: (i, 0, 0)),
            fixed(padded, LANES), fixed(padded, LANES), fixed(padded, LANES), fixed(1, LANES),
            fixed(2 * padded, padded), fixed(reactions, 2 * LANES), fixed(2 * padded, reactions),
        ],
        out_shape=[
            shape(row_count, padded, LANES), shape(row_count, padded, LANES),
            shape(padded, LANES), shape(padded, LANES), shape(padded, LANES), shape(1, LANES),
            shape(2 * padded, padded, dtype=BF16), shape(reactions, 2 * LANES, dtype=BF16),
            shape(2 * padded, reactions, dtype=BF16),
        ],
        scratch_shapes=[
            pltpu.VMEM((padded, LANES), F32), pltpu.VMEM((LANES, across), F32),
            pltpu.VMEM((reactions, LANES), F32), pltpu.VMEM((padded, reactions), F32),
        ],
        compiler_params=pltpu.CompilerParams(vmem_limit_bytes=24 * 2**20),
        name="spread",
    )(
        levels.transpose(1, 0, 2), heat, inverse, factor.reshape(1, -1), exponents,
        energies.reshape(1, -1), change,
    )

    def neighbour(value, axis, ahead):
        count = lax.axis_size(axis)
        pairs = [(i, i + 1) if ahead else (i + 1, i) for i in range(count - 1)]
        return lax.ppermute(value, axis, pairs)

    up = neighbour(bottom, FLOW, True)
    down = neighbour(top, FLOW, False)
    left = neighbour(cols, "chem", True)
    right = neighbour(cols, "chem", False)
    peaks = lax.all_to_all(peak.reshape(-1), FLOW_CHEM, 0, 0, tiled=True).reshape(1, -1)

    wide = GROUP * LANES
    out, heat_out = pl.pallas_call(
        functools.partial(advance_kernel, species, reactions),
        in_specs=[pl.BlockSpec(memory_space=pltpu.SMEM)] + [whole] * 13,
        out_specs=[pl.BlockSpec(memory_space=pl.ANY), whole],
        out_shape=[shape(species, row_count, LANES), shape(row_count, LANES)],
        scratch_shapes=[
            pltpu.VMEM((row_count, padded, LANES), F32),
            pltpu.VMEM((padded, LANES), F32),
            pltpu.VMEM((2, padded, LANES), F32),
            pltpu.VMEM((padded, LANES), F32),
            pltpu.SMEM((row_count + 1,), jnp.int32),
            pltpu.VMEM((padded, wide), F32),
            pltpu.VMEM((padded, wide), F32),
            pltpu.VMEM((padded, wide), F32),
            pltpu.VMEM((4 * LANES, wide), BF16),
            pltpu.VMEM((reactions, wide), BF16),
            pltpu.VMEM((reactions, wide), BF16),
            pltpu.VMEM((padded, LANES), F32),
            pltpu.SemaphoreType.DMA((2,)),
        ],
        compiler_params=pltpu.CompilerParams(vmem_limit_bytes=40 * 2**20),
        name="advance",
    )(
        flags.reshape(-1), peaks, cells, spread, up, down, left, right, cols, heat,
        stacked, table, matrix, jnp.pad(cooling, (0, padded - species)).reshape(-1, 1),
    )
    return out.transpose(1, 0, 2), heat_out


def solution(mesh):
    torus = Mesh(
        mesh.devices.reshape(4, 4, 2, mesh.shape["chem"]), ("flow_0", "flow_1", "flow_2", "chem")
    )
    placed = (P(FLOW, None, "chem"), P(FLOW, "chem"), P(), P(), P(), P(), P(), P(), P(FLOW, "chem"))
    return jax.shard_map(
        per_device,
        mesh=torus,
        in_specs=placed,
        out_specs=(P(FLOW, None, "chem"), P(FLOW, "chem")),
        check_vma=False,
    )
```

```python
import functools

import jax
import jax.numpy as jnp
from jax import lax
from jax.experimental import pallas as pl
from jax.experimental.pallas import tpu as pltpu
from jax.sharding import Mesh
from jax.sharding import PartitionSpec as P

FLOW = ("flow_0", "flow_1", "flow_2")
FLOW_CHEM = ("flow_0", "flow_1", "flow_2", "chem")

COURANT = 0.2
CHEM_STEP = 0.05
LOG_OFFSET = 0.001
RATE_CEILING = 2.0
LOG2E = 1.4426950408889634

F32 = jnp.float32
BF16 = jnp.bfloat16
LANES = 128
GROUP = 4
CHUNK = 8
HALF = 4


def split2(value):
    high = value.astype(BF16)
    return high, (value - high.astype(F32)).astype(BF16)


def split3(value):
    high = value.astype(BF16)
    rest = value - high.astype(F32)
    mid = rest.astype(BF16)
    return high, mid, (rest - mid.astype(F32)).astype(BF16)


def mxu(lhs, rhs):
    return jnp.dot(lhs, rhs, preferred_element_type=F32)


def mixture(cells, stacked):
    padded = cells.shape[0]
    high, low = split2(cells)
    both = mxu(stacked[...], high)
    total = both[:padded] + both[padded:] + mxu(stacked[0:padded], low)
    heat = cells[padded - 1 : padded]
    there = heat > 0.0
    scaled = heat * jnp.sqrt(heat)
    return jnp.where(there, scaled, 0.0) / jnp.where(there, total, 1.0)


def lane_index(shape):
    return lax.broadcasted_iota(jnp.int32, shape, len(shape) - 1)


def spread_kernel(
    species, reactions,
    x_hbm, t_hbm, r_hbm, a_ref, k_hbm, e_ref, m_hbm, cool_ref,
    c_hbm, d_hbm, even_ref, odd_ref, cols_ref, peak_ref, rs_ref, ka_ref, ms_ref, mr_ref, cool_col,
    x_buf, c_buf, d_buf, heat, square, rows, tall, wide, first_col, last_col, in_sems, small_sems, out_sem,
):
    row_count, padded, _ = c_buf.shape
    chunks = row_count // CHUNK
    full = ms_ref.shape[1]

    def chunk_in(i):
        return pltpu.make_async_copy(x_hbm.at[:, pl.ds(i * CHUNK, CHUNK)], x_buf.at[i], in_sems.at[i])

    heat_in = pltpu.make_async_copy(t_hbm, heat, small_sems.at[0])
    heat_in.start()
    chunk_in(0).start()
    inverse_in = pltpu.make_async_copy(r_hbm, square, small_sems.at[1])
    inverse_in.start()
    for i in range(1, chunks):
        chunk_in(i).start()
    exponents_in = pltpu.make_async_copy(k_hbm, tall, small_sems.at[2])
    exponents_in.start()
    change_in = pltpu.make_async_copy(m_hbm, wide, small_sems.at[3])
    change_in.start()

    rows[...] = jnp.zeros_like(rows)
    factors = split3(a_ref[...].reshape(1, reactions) * LOG2E)
    energies = split3(e_ref[...].reshape(1, reactions) * LOG2E)
    order = [factors[0], factors[1], factors[2]] + [energies[i] for i in (0, 0, 0, 1, 1, 2)]
    for i, row in enumerate(order):
        rows[padded + i : padded + i + 1, 0:reactions] = row.astype(F32)
    rows[0:1, reactions : reactions + species] = cool_ref[...].reshape(1, species)

    inverse_in.wait()
    high, low = split2(square[...])
    none = jnp.zeros((species, padded - species), BF16)
    for first, part in ((0, high), (padded, low)):
        part = jnp.concatenate([part, none], axis=1)
        rs_ref[first : first + padded] = jnp.concatenate([part, part[0 : padded - species]], axis=0)

    heat_in.wait()
    lane = lane_index((padded, LANES))
    def chunk(i, peak):
        chunk_in(i).wait()
        flat = x_buf.at[i].reshape(species * CHUNK, LANES)
        base = i * CHUNK
        first = jnp.zeros((padded, LANES), F32)
        last = jnp.zeros((padded, LANES), F32)
        for pair in range(0, CHUNK, 2):
            for r in (pair, pair + 1):
                c_buf[base + r, 0:species] = flat[pl.ds(r, species, stride=CHUNK), :]
                c_buf[base + r, species:padded] = heat[pl.ds(base + r, 1), :]
            cells = jnp.concatenate([c_buf[base + pair], c_buf[base + pair + 1]], axis=1)
            spread = mixture(cells, rs_ref)
            d_buf[base + pair] = spread[:, 0:LANES]
            d_buf[base + pair + 1] = spread[:, LANES:]
            peak = jnp.maximum(peak, jnp.maximum(spread[:, 0:LANES], spread[:, LANES:]))
            for r in (pair, pair + 1):
                row = cells[:, (r - pair) * LANES : (r - pair + 1) * LANES]
                row = pltpu.roll(row, r, 1) if r else row
                first = jnp.where(lane == r, row, first)
                last = jnp.where(lane == (r - 1) % LANES, row, last)
        here = lane // CHUNK == i
        first_col[...] = jnp.where(here, pltpu.roll(first, base, 1), first_col[...])
        last_col[...] = jnp.where(here, pltpu.roll(last, base + 1, 1), last_col[...])
        rows_here = pl.ds(base, CHUNK)
        pltpu.make_async_copy(c_buf.at[rows_here], c_hbm.at[rows_here], out_sem).start()
        pltpu.make_async_copy(d_buf.at[rows_here], d_hbm.at[rows_here], out_sem).start()
        return peak

    first_col[...] = jnp.zeros_like(first_col)
    last_col[...] = jnp.zeros_like(last_col)
    peak = lax.fori_loop(0, chunks, chunk, jnp.zeros((padded, LANES), F32))
    best = jnp.max(jnp.max(peak, axis=0, keepdims=True), axis=1, keepdims=True)
    peak_ref[...] = jnp.broadcast_to(best, peak_ref.shape)
    cols_ref[...] = jnp.where(lane < 64, first_col[...], pltpu.roll(last_col[...], 64, 1))
    flipped = lax.axis_index(FLOW[-1]) * (row_count - 1)
    even_ref[...] = c_buf[row_count - 1 - flipped]
    odd_ref[...] = c_buf[flipped]

    exponents_in.wait()
    for start in range(0, reactions, LANES):
        size = min(LANES, reactions - start)
        turned = rows[:, start : start + LANES].T[0:size]
        high, low = split2(tall[start : start + size, :])
        none = jnp.zeros((size, LANES - species), BF16)
        spare = lane_index((size, LANES)) >= padded
        high = jnp.concatenate([high, none], axis=1)
        ka_ref[start : start + size, 0:LANES] = jnp.where(spare, turned.astype(BF16), high)
        ka_ref[start : start + size, LANES : 2 * LANES] = jnp.concatenate([low, none], axis=1)
    cool_col[...] = jnp.broadcast_to(rows[:, reactions : reactions + LANES].T[0:padded, 0:1], cool_col.shape)
    change_in.wait()
    high, low = split2(wide[...])
    none = jnp.zeros((padded - species, reactions), BF16)
    high = jnp.concatenate([high, none], axis=0)
    low = jnp.concatenate([low, none], axis=0)
    ms_ref[0:padded] = high[:, 0:full]
    ms_ref[padded : 2 * padded] = low[:, 0:full]
    mr_ref[...] = jnp.concatenate([high[:, full:], low[:, full:], high[:, full:]], axis=1)

    pltpu.make_async_copy(c_buf, c_hbm, out_sem).wait()
    pltpu.make_async_copy(d_buf, d_hbm, out_sem).wait()


def flux_kernel(
    c_hbm, d_hbm, even_ref, odd_ref, pair_ref, cross_ref, cols_ref, rs_ref, s_hbm,
    c_ref, d_ref, s_ref, first_ref, last_ref, gap_ref, step_ref, in_sems, out_sem,
):
    row_count, padded, _ = s_ref.shape
    chunks = row_count // CHUNK
    lane = lane_index((padded, LANES))

    def chunk_in(i):
        here = pl.ds(i * CHUNK, CHUNK)
        return (
            pltpu.make_async_copy(c_hbm.at[here], c_ref.at[here], in_sems.at[0, i]),
            pltpu.make_async_copy(d_hbm.at[here], d_ref.at[here], in_sems.at[1, i]),
        )

    for i in range(chunks):
        for copy in chunk_in(i):
            copy.start()

    odd = lax.axis_index(FLOW[-1]) == 1
    above = jnp.where(odd, even_ref[...], odd_ref[...])
    below = jnp.where(odd, odd_ref[...], even_ref[...])
    odd = lax.rem(lax.axis_index("chem"), 2) == 1
    left = jnp.where(odd, pair_ref[...], cross_ref[...])
    right = jnp.where(odd, cross_ref[...], pair_ref[...])
    beyond = pltpu.roll(jnp.where(lane < 64, right, left), 64, 1)
    mine = cols_ref[...]
    spread = mixture(jnp.concatenate([mine, beyond], axis=1), rs_ref)
    edge = (spread[:, 0:LANES] + spread[:, LANES:]) * (beyond - mine)
    first_ref[...] = edge
    last_ref[...] = pltpu.roll(edge, 63, 1)
    outer = mixture(jnp.concatenate([above, below], axis=1), rs_ref)
    c_ref[row_count] = below
    d_ref[row_count] = outer[:, LANES:]

    rows = jnp.bitwise_and(lax.broadcasted_iota(jnp.int32, (2 * LANES, 2 * LANES), 0), LANES - 1)
    cell = lane_index((2 * LANES, 2 * LANES))
    back = cell >= LANES
    cell = jnp.bitwise_and(cell, LANES - 1)
    beside = jnp.where(back, cell - 1, cell + 1)
    inside = jnp.logical_and(beside >= 0, beside < LANES)
    there = jnp.where(jnp.logical_and(inside, rows == beside), 1.0, 0.0)
    here = jnp.where(jnp.logical_and(inside, rows == cell), 1.0, 0.0)
    step_ref[0] = (there - here).astype(BF16)
    step_ref[1] = (there + here).astype(BF16)

    def wait_in(i):
        for copy in chunk_in(i):
            copy.wait()

    def beside_of(ref, base, which):
        value = ref[pl.ds(base, HALF)].reshape(HALF * padded, LANES)
        return mxu(jnp.concatenate(split2(value), axis=1), step_ref[which])

    wait_in(0)
    gap_ref[...] = (d_ref[0] + outer[:, 0:LANES]) * (c_ref[0] - above)

    @pl.loop(0, row_count // HALF)
    def _(part):
        base = part * HALF

        @pl.when(jnp.logical_and(part % 2 == 1, part < row_count // HALF - 1))
        def _():
            wait_in(part // 2 + 1)

        change = beside_of(c_ref, base, 0)
        total = beside_of(d_ref, base, 1)
        along = change * total
        along = along[:, 0:LANES] + along[:, LANES:]
        gap = gap_ref[...]
        for r in range(HALF):
            x = base + r
            later = (d_ref[x] + d_ref[x + 1]) * (c_ref[x + 1] - c_ref[x])
            ends = pltpu.roll(jnp.where(lane == x, first_ref[...], last_ref[...]), LANES - x, 1)
            ends = jnp.where(jnp.logical_or(lane == 0, lane == LANES - 1), ends, 0.0)
            s_ref[x] = (along[r * padded : (r + 1) * padded] + ends) + (later - gap)
            gap = later
        gap_ref[...] = gap

        @pl.when(part % 2 == 1)
        def _():
            done = pl.ds((part // 2) * CHUNK, CHUNK)
            pltpu.make_async_copy(s_ref.at[done], s_hbm.at[done], out_sem).start()

    pltpu.make_async_copy(s_ref, s_hbm, out_sem).wait()


def advance_kernel(
    species, reactions,
    flag_ref, peak_ref, c_hbm, s_hbm, ka_ref, ms_ref, mr_ref, cool_col,
    out_hbm, heat_ref,
    c_ref, s_ref, o_ref, order_ref, base_ref, k_ref, sum_ref, log_ref, high_ref, low_ref, rest_ref,
    in_sems, out_sem,
):
    row_count, padded, _ = c_ref.shape
    full = high_ref.shape[0]
    chunks = row_count // CHUNK

    def chunk_in(i):
        here = pl.ds(i * CHUNK, CHUNK)
        return (
            pltpu.make_async_copy(c_hbm.at[here], c_ref.at[here], in_sems.at[0, i]),
            pltpu.make_async_copy(s_hbm.at[here], s_ref.at[here], in_sems.at[1, i]),
        )

    for i in range(chunks):
        for copy in chunk_in(i):
            copy.start()

    def gather(x, found):
        order_ref[found] = x
        return found + flag_ref[x]

    live = lax.fori_loop(0, row_count, gather, jnp.int32(0))
    order_ref[live] = row_count

    largest = jnp.max(jnp.max(peak_ref[...], axis=0, keepdims=True), axis=1, keepdims=True)
    half_step = jnp.broadcast_to(0.5 * (COURANT / largest), (padded, LANES))
    flat_out = o_ref.reshape(row_count * species, LANES)

    def put(x, value):
        first = (x // CHUNK) * (CHUNK * species) + jnp.bitwise_and(x, CHUNK - 1)
        flat_out[pl.ds(first, species, stride=CHUNK), :] = value[0:species]

    @pl.loop(0, chunks)
    def _(i):
        for copy in chunk_in(i):
            copy.wait()
        for r in range(CHUNK):
            x = i * CHUNK + r
            value = c_ref[x] + half_step * s_ref[x]
            c_ref[x, 0:species] = value[0:species]
            flat_out[pl.ds(i * (CHUNK * species) + r, species, stride=CHUNK), :] = value[0:species]
            heat_ref[pl.ds(x, 1), :] = c_ref[x, padded - 1 : padded]

    def send(i, _):
        pltpu.make_async_copy(o_ref.at[i], out_hbm.at[:, pl.ds(i * CHUNK, CHUNK)], out_sem).start()
        return 0

    sent = order_ref[0] // CHUNK
    lax.fori_loop(0, sent, send, 0)

    log_ref[...] = jnp.zeros_like(log_ref)
    ceiling = RATE_CEILING * LOG2E

    def production(state):
        high, low = split2(jnp.log2(jnp.abs(state) + LOG_OFFSET))
        log_ref[0:padded] = high
        log_ref[LANES : LANES + padded] = high
        log_ref[2 * LANES : 2 * LANES + padded] = low
        log_ref[3 * LANES : 3 * LANES + padded] = low
        for start in range(0, reactions, LANES):
            size = min(LANES, reactions - start)
            table = ka_ref[start : start + size]
            rate = mxu(table, log_ref[0 : 2 * LANES]) + mxu(table, log_ref[2 * LANES : 4 * LANES])
            high, low = split2(jnp.exp2(jnp.minimum(rate, ceiling)))
            if start < full:
                high_ref[start : start + size] = high
                low_ref[start : start + size] = low
            else:
                rest_ref[...] = jnp.concatenate([high, high, low], axis=0)
        both = mxu(ms_ref[...], high_ref[...])
        return (both[0:padded] + both[padded:]) + mxu(ms_ref[0:padded], low_ref[...]) + mxu(mr_ref[...], rest_ref[...])

    @pl.loop(0, (live + GROUP - 1) // GROUP, init_carry=sent)
    def sent(group, sent):
        places = [order_ref[jnp.minimum(group * GROUP + i, live - 1)] for i in range(GROUP)]
        for i, x in enumerate(places):
            base_ref[:, i * LANES : (i + 1) * LANES] = c_ref[x]
        heat = base_ref[padded - 1 : padded]
        parts = split3(-1.0 / heat)
        one = jnp.ones_like(parts[0])
        zero = jnp.zeros_like(one)
        extra = [one, one, one] + [parts[i] for i in (0, 1, 2, 0, 1, 0)] + [zero] * 7
        log_ref[padded:LANES] = jnp.concatenate(extra, axis=0)

        k_ref[...] = production(base_ref[...])
        sum_ref[...] = k_ref[...]
        k_ref[...] = production(base_ref[...] + 0.5 * CHEM_STEP * k_ref[...])
        sum_ref[...] += 2.0 * k_ref[...]
        k_ref[...] = production(base_ref[...] + 0.5 * CHEM_STEP * k_ref[...])
        sum_ref[...] += 2.0 * k_ref[...]
        total = sum_ref[...] + production(base_ref[...] + CHEM_STEP * k_ref[...])
        result = base_ref[...] + CHEM_STEP / 6.0 * total
        moved = result - base_ref[...]
        for i, x in enumerate(places):
            lanes = slice(i * LANES, (i + 1) * LANES)
            put(x, result[:, lanes])
            drop = jnp.sum(cool_col[...] * moved[:, lanes], axis=0, keepdims=True)
            heat_ref[pl.ds(x, 1), :] = base_ref[padded - 1 : padded, lanes] - drop

        done = order_ref[jnp.minimum(group * GROUP + GROUP, live)] // CHUNK
        lax.fori_loop(sent, done, send, 0)
        return done

    lax.fori_loop(sent, chunks, send, 0)

    def wait_out(i, _):
        pltpu.make_async_copy(o_ref.at[0], out_hbm.at[:, pl.ds(0, CHUNK)], out_sem).wait()
        return 0

    lax.fori_loop(0, chunks, wait_out, 0)


def per_device(levels, heat, inverse, factor, exponents, energies, change, cooling, flags):
    row_count, species, _ = levels.shape
    reactions = factor.shape[0]
    padded = -(-species // 16) * 16
    across = -(-reactions // LANES) * LANES + LANES
    chunks = row_count // CHUNK
    full = reactions // LANES * LANES
    rest = reactions - full
    devices = 1
    for axis in FLOW_CHEM:
        devices *= lax.axis_size(axis)
    near = pl.BlockSpec(memory_space=pltpu.VMEM)
    far = pl.BlockSpec(memory_space=pltpu.HBM)

    def shape(*dims, dtype=F32):
        return jax.ShapeDtypeStruct(dims, dtype)

    plane = (row_count, padded, LANES)
    cells, spread, even, odd, cols, peak, stacked, table, matrix, narrow, cool_col = pl.pallas_call(
        functools.partial(spread_kernel, species, reactions),
        in_specs=[far, far, far, near, far, near, far, near],
        out_specs=[far, far] + [near] * 9,
        out_shape=[
            shape(*plane), shape(*plane),
            shape(padded, LANES), shape(padded, LANES), shape(padded, LANES), shape(devices, LANES),
            shape(2 * padded, padded, dtype=BF16), shape(reactions, 2 * LANES, dtype=BF16),
            shape(2 * padded, full, dtype=BF16), shape(padded, 3 * rest, dtype=BF16), shape(padded, LANES),
        ],
        scratch_shapes=[
            pltpu.VMEM((chunks, species, CHUNK, LANES), F32), pltpu.VMEM(plane, F32), pltpu.VMEM(plane, F32),
            pltpu.VMEM((row_count, LANES), F32), pltpu.VMEM((species, species), F32),
            pltpu.VMEM((LANES, across), F32), pltpu.VMEM((reactions, species), F32),
            pltpu.VMEM((species, reactions), F32),
            pltpu.VMEM((padded, LANES), F32), pltpu.VMEM((padded, LANES), F32),
            pltpu.SemaphoreType.DMA((chunks,)), pltpu.SemaphoreType.DMA((4,)), pltpu.SemaphoreType.DMA,
        ],
        cost_estimate=pl.CostEstimate(flops=10**9, bytes_accessed=11 * 10**6, transcendentals=0),
        name="spread",
    )(levels.transpose(1, 0, 2), heat, inverse, factor, exponents, energies, change, cooling)

    def swap(value, axis, first):
        pairs = []
        for i in range(first, lax.axis_size(axis) - 1, 2):
            pairs += [(i, i + 1), (i + 1, i)]
        return lax.ppermute(value, axis, pairs)

    peaks = lax.all_to_all(peak, FLOW_CHEM, 0, 0, tiled=True)
    even = swap(even, FLOW, 0)
    odd = swap(odd, FLOW, 1)
    pair = swap(cols, "chem", 0)
    cross = swap(cols, "chem", 1)

    fluxes = pl.pallas_call(
        flux_kernel,
        in_specs=[far, far] + [near] * 6,
        out_specs=far,
        out_shape=shape(*plane),
        scratch_shapes=[
            pltpu.VMEM((row_count + 1, padded, LANES), F32), pltpu.VMEM((row_count + 1, padded, LANES), F32),
            pltpu.VMEM(plane, F32), pltpu.VMEM((padded, LANES), F32), pltpu.VMEM((padded, LANES), F32),
            pltpu.VMEM((padded, LANES), F32), pltpu.VMEM((2, 2 * LANES, 2 * LANES), BF16),
            pltpu.SemaphoreType.DMA((2, chunks)), pltpu.SemaphoreType.DMA,
        ],
        cost_estimate=pl.CostEstimate(flops=10**9, bytes_accessed=11 * 10**6, transcendentals=0),
        name="flux",
    )(cells, spread, even, odd, pair, cross, cols, stacked)

    span = GROUP * LANES
    out, heat_out = pl.pallas_call(
        functools.partial(advance_kernel, species, reactions),
        in_specs=[pl.BlockSpec(memory_space=pltpu.SMEM), near, far, far, near, near, near, near],
        out_specs=[far, near],
        out_shape=[shape(species, row_count, LANES), shape(row_count, LANES)],
        scratch_shapes=[
            pltpu.VMEM(plane, F32), pltpu.VMEM(plane, F32), pltpu.VMEM((chunks, species, CHUNK, LANES), F32),
            pltpu.SMEM((row_count + 1,), jnp.int32),
            pltpu.VMEM((padded, span), F32), pltpu.VMEM((padded, span), F32), pltpu.VMEM((padded, span), F32),
            pltpu.VMEM((4 * LANES, span), BF16),
            pltpu.VMEM((full, span), BF16), pltpu.VMEM((full, span), BF16), pltpu.VMEM((3 * rest, span), BF16),
            pltpu.SemaphoreType.DMA((2, chunks)), pltpu.SemaphoreType.DMA,
        ],
        cost_estimate=pl.CostEstimate(flops=2 * 10**10, bytes_accessed=11 * 10**6, transcendentals=0),
        name="advance",
    )(flags.reshape(-1), peaks, cells, fluxes, table, matrix, narrow, cool_col)
    return out.transpose(1, 0, 2), heat_out


def solution(mesh):
    torus = Mesh(
        mesh.devices.reshape(4, 4, 2, mesh.shape["chem"]), ("flow_0", "flow_1", "flow_2", "chem")
    )
    placed = (P(FLOW, None, "chem"), P(FLOW, "chem"), P(), P(), P(), P(), P(), P(), P(FLOW, "chem"))
    return jax.shard_map(
        per_device,
        mesh=torus,
        in_specs=placed,
        out_specs=(P(FLOW, None, "chem"), P(FLOW, "chem")),
        check_vma=False,
    )
```

```python
import functools

import jax
import jax.numpy as jnp
from jax import lax
from jax.experimental import pallas as pl
from jax.experimental.pallas import tpu as pltpu
from jax.sharding import Mesh
from jax.sharding import PartitionSpec as P

FLOW = ("flow_0", "flow_1", "flow_2")
FLOW_CHEM = ("flow_0", "flow_1", "flow_2", "chem")

COURANT = 0.2
CHEM_STEP = 0.05
LOG_OFFSET = 0.001
RATE_CEILING = 2.0
LOG2E = 1.4426950408889634

F32 = jnp.float32
BF16 = jnp.bfloat16
LANES = 128
GROUP = 4
STREAMS = 2
SPAN = 784
CHUNK = 8
HALF = 4


def split2(value):
    high = value.astype(BF16)
    return high, (value - high.astype(F32)).astype(BF16)


def split3(value):
    high = value.astype(BF16)
    rest = value - high.astype(F32)
    mid = rest.astype(BF16)
    return high, mid, (rest - mid.astype(F32)).astype(BF16)


def mxu(lhs, rhs):
    return jnp.dot(lhs, rhs, preferred_element_type=F32)


def mixture(cells, stacked):
    padded = cells.shape[0]
    high, low = split2(cells)
    both = mxu(stacked[...], high)
    total = both[:padded] + both[padded:] + mxu(stacked[0:padded], low)
    heat = cells[padded - 1 : padded]
    there = heat > 0.0
    scaled = heat * jnp.sqrt(heat)
    return jnp.where(there, scaled, 0.0) / jnp.where(there, total, 1.0)


def lane_index(shape):
    return lax.broadcasted_iota(jnp.int32, shape, len(shape) - 1)


def stack_inverse(stacked, inverse):
    species = inverse.shape[0]
    padded = stacked.shape[0] // 2
    none = jnp.zeros((species, padded - species), BF16)
    for first, part in zip((0, padded), split2(inverse[...])):
        part = jnp.concatenate([part, none], axis=1)
        stacked[first : first + padded] = jnp.concatenate([part, part[0 : padded - species]], axis=0)


def spread_kernel(
    species,
    x_hbm, t_hbm, r_hbm,
    c_hbm, d_hbm, even_hbm, odd_hbm, cols_hbm, peak_hbm,
    cols_ref, peak_ref, x_buf, c_buf, d_buf, heat, square, rs_ref, first_col, last_col, in_sems, small_sems, end_sems, out_sem,
):
    row_count, padded, _ = c_buf.shape
    chunks = row_count // CHUNK

    def chunk_in(i):
        return pltpu.make_async_copy(x_hbm.at[:, pl.ds(i * CHUNK, CHUNK)], x_buf.at[i], in_sems.at[i])

    chunk_in(0).start()
    heat_in = pltpu.make_async_copy(t_hbm, heat, small_sems.at[0])
    heat_in.start()
    inverse_in = pltpu.make_async_copy(r_hbm, square, small_sems.at[1])
    inverse_in.start()
    for i in range(1, chunks):
        chunk_in(i).start()

    first_col[...] = jnp.zeros_like(first_col)
    last_col[...] = jnp.zeros_like(last_col)
    lane = lane_index((padded, LANES))
    inverse_in.wait()
    stack_inverse(rs_ref, square)
    heat_in.wait()

    def send(buf, hbm, i):
        here = pl.ds(i * CHUNK, CHUNK)
        pltpu.make_async_copy(buf.at[here], hbm.at[here], out_sem).start()

    def chunk(i, peak):
        chunk_in(i).wait()
        flat = x_buf.at[i].reshape(species * CHUNK, LANES)
        base = i * CHUNK
        first = jnp.zeros((padded, LANES), F32)
        last = jnp.zeros((padded, LANES), F32)
        for pair in range(0, CHUNK, 2):
            x = base + pair
            for r in (pair, pair + 1):
                c_buf[base + r, 0:species] = flat[pl.ds(r, species, stride=CHUNK), :]
                c_buf[base + r, species:padded] = heat[pl.ds(base + r, 1), :]
            row = [c_buf[x], c_buf[x + 1]]
            high, low = split2(jnp.concatenate(row, axis=1))
            both = mxu(rs_ref[...], high)
            total = both[:padded] + both[padded:] + mxu(rs_ref[0:padded], low)
            warm = jnp.concatenate([heat[pl.ds(x, 1), :], heat[pl.ds(x + 1, 1), :]], axis=1)
            spread = warm * jnp.sqrt(warm) / total
            thin = [spread[:, 0:LANES], spread[:, LANES:]]
            peak = jnp.maximum(peak, jnp.maximum(thin[0], thin[1]))

            d_buf[x] = thin[0]
            d_buf[x + 1] = thin[1]
            for r, value in zip((pair, pair + 1), row):
                value = pltpu.roll(value, r, 1) if r else value
                first = jnp.where(lane == r, value, first)
                last = jnp.where(lane == (r - 1) % LANES, value, last)
        here = lane // CHUNK == i
        first_col[...] = jnp.where(here, pltpu.roll(first, base, 1), first_col[...])
        last_col[...] = jnp.where(here, pltpu.roll(last, base + 1, 1), last_col[...])
        send(c_buf, c_hbm, i)
        send(d_buf, d_hbm, i)
        return peak

    peak = lax.fori_loop(0, chunks, chunk, jnp.zeros((padded, LANES), F32))
    best = jnp.max(jnp.max(peak, axis=0, keepdims=True), axis=1, keepdims=True)
    peak_ref[...] = jnp.broadcast_to(best, peak_ref.shape)
    cols_ref[...] = jnp.where(lane < 64, first_col[...], pltpu.roll(last_col[...], 64, 1))
    flipped = lax.axis_index(FLOW[-1]) * (row_count - 1)
    ends = [
        pltpu.make_async_copy(src, dst, end_sems.at[n])
        for n, (src, dst) in enumerate((
            (peak_ref, peak_hbm), (cols_ref, cols_hbm),
            (c_buf.at[row_count - 1 - flipped], even_hbm), (c_buf.at[flipped], odd_hbm),
        ))
    ]
    for copy in ends:
        copy.start()
    for copy in ends:
        copy.wait()
    pltpu.make_async_copy(c_buf, c_hbm, out_sem).wait()
    pltpu.make_async_copy(d_buf, d_hbm, out_sem).wait()


def flux_kernel(
    c_hbm, d_hbm, even_hbm, odd_hbm, pair_hbm, cross_hbm, cols_hbm, r_hbm, s_hbm,
    c_ref, d_ref, s_ref, sides, square, rs_ref, first_ref, last_ref, gap_ref, step_ref, in_sems, small_sems, out_sem,
):
    row_count, padded, _ = s_ref.shape
    chunks = row_count // CHUNK
    lane = lane_index((padded, LANES))

    def chunk_in(i):
        here = pl.ds(i * CHUNK, CHUNK)
        return (
            pltpu.make_async_copy(c_hbm.at[here], c_ref.at[here], in_sems.at[0, i]),
            pltpu.make_async_copy(d_hbm.at[here], d_ref.at[here], in_sems.at[1, i]),
        )

    small = [pltpu.make_async_copy(r_hbm, square, small_sems.at[0])]
    for n, side in enumerate((even_hbm, odd_hbm, pair_hbm, cross_hbm, cols_hbm)):
        small.append(pltpu.make_async_copy(side, sides.at[n], small_sems.at[n + 1]))
    for copy in small:
        copy.start()
    for i in range(chunks):
        for copy in chunk_in(i):
            copy.start()

    rows = jnp.bitwise_and(lax.broadcasted_iota(jnp.int32, (2 * LANES, 2 * LANES), 0), LANES - 1)
    cell = lane_index((2 * LANES, 2 * LANES))
    back = cell >= LANES
    cell = jnp.bitwise_and(cell, LANES - 1)
    beside = jnp.where(back, cell - 1, cell + 1)
    inside = jnp.logical_and(beside >= 0, beside < LANES)
    there = jnp.where(jnp.logical_and(inside, rows == beside), 1.0, 0.0)
    here = jnp.where(jnp.logical_and(inside, rows == cell), 1.0, 0.0)
    step_ref[0] = (there - here).astype(BF16)
    step_ref[1] = (there + here).astype(BF16)
    for copy in small:
        copy.wait()
    stack_inverse(rs_ref, square)

    odd = lax.axis_index(FLOW[-1]) == 1
    above = jnp.where(odd, sides[0], sides[1])
    below = jnp.where(odd, sides[1], sides[0])
    odd = lax.rem(lax.axis_index("chem"), 2) == 1
    left = jnp.where(odd, sides[2], sides[3])
    right = jnp.where(odd, sides[3], sides[2])
    beyond = pltpu.roll(jnp.where(lane < 64, right, left), 64, 1)
    mine = sides[4]
    spread = mixture(jnp.concatenate([mine, beyond], axis=1), rs_ref)
    edge = (spread[:, 0:LANES] + spread[:, LANES:]) * (beyond - mine)
    first_ref[...] = edge
    last_ref[...] = pltpu.roll(edge, 63, 1)
    outer = mixture(jnp.concatenate([above, below], axis=1), rs_ref)
    c_ref[row_count] = below
    d_ref[row_count] = outer[:, LANES:]

    def wait_in(i):
        for copy in chunk_in(i):
            copy.wait()

    def beside_of(ref, base, which):
        value = ref[pl.ds(base, HALF)].reshape(HALF * padded, LANES)
        return mxu(jnp.concatenate(split2(value), axis=1), step_ref[which])

    wait_in(0)
    gap_ref[...] = (d_ref[0] + outer[:, 0:LANES]) * (c_ref[0] - above)

    @pl.loop(0, row_count // HALF)
    def _(part):
        base = part * HALF

        @pl.when(jnp.logical_and(part % 2 == 1, part < row_count // HALF - 1))
        def _():
            wait_in(part // 2 + 1)

        change = beside_of(c_ref, base, 0)
        total = beside_of(d_ref, base, 1)
        along = change * total
        along = along[:, 0:LANES] + along[:, LANES:]
        gap = gap_ref[...]
        for r in range(HALF):
            x = base + r
            later = (d_ref[x] + d_ref[x + 1]) * (c_ref[x + 1] - c_ref[x])
            ends = pltpu.roll(jnp.where(lane == x, first_ref[...], last_ref[...]), LANES - x, 1)
            ends = jnp.where(jnp.logical_or(lane == 0, lane == LANES - 1), ends, 0.0)
            s_ref[x] = (along[r * padded : (r + 1) * padded] + ends) + (later - gap)
            gap = later
        gap_ref[...] = gap

        @pl.when(part % 2 == 1)
        def _():
            done = pl.ds((part // 2) * CHUNK, CHUNK)
            pltpu.make_async_copy(s_ref.at[done], s_hbm.at[done], out_sem).start()

    pltpu.make_async_copy(s_ref, s_hbm, out_sem).wait()


def advance_kernel(
    species, reactions,
    flag_hbm, peak_hbm, c_hbm, s_hbm, a_hbm, k_hbm, e_hbm, m_hbm, cool_hbm,
    out_hbm, heat_hbm,
    flag_ref, a_ref, e_ref, cool_ref, heat_ref, c_ref, s_ref, o_ref, order_ref, half_ref, peaks, rows, tall, wide,
    ka_ref, ms_ref, mr_ref, cool_col, small_sems, early_sems, heat_sem, *rest,
):
    streams = [rest[i * 7 : i * 7 + 7] for i in range(STREAMS)]
    in_sems, out_sem = rest[STREAMS * 7 :]
    row_count, padded, _ = c_ref.shape
    full = ms_ref.shape[1]
    chunks = row_count // CHUNK
    together = STREAMS * GROUP

    def chunk_in(i):
        here = pl.ds(i * CHUNK, CHUNK)
        return (
            pltpu.make_async_copy(c_hbm.at[here], c_ref.at[here], in_sems.at[0, i]),
            pltpu.make_async_copy(s_hbm.at[here], s_ref.at[here], in_sems.at[1, i]),
        )

    small = [
        pltpu.make_async_copy(*ends, small_sems.at[n])
        for n, ends in enumerate(
            ((peak_hbm, peaks), (k_hbm, tall), (m_hbm, wide))
        )
    ]
    early = [
        pltpu.make_async_copy(*ends, early_sems.at[n])
        for n, ends in enumerate(((flag_hbm, flag_ref), (a_hbm, a_ref), (e_hbm, e_ref), (cool_hbm, cool_ref)))
    ]
    for copy in early:
        copy.start()
    for copy in small:
        copy.start()
    for i in range(chunks):
        for copy in chunk_in(i):
            copy.start()

    rows[...] = jnp.zeros_like(rows)
    for stream in streams:
        stream[3][...] = jnp.zeros_like(stream[3])
    for copy in early:
        copy.wait()
    factors = split3(a_ref[...].reshape(1, reactions) * LOG2E)
    energies = split3(e_ref[...].reshape(1, reactions) * LOG2E)
    order = [factors[0], factors[1], factors[2]] + [energies[i] for i in (0, 0, 0, 1, 1, 2)]
    for i, row in enumerate(order):
        rows[padded + i : padded + i + 1, 0:reactions] = row.astype(F32)
    rows[0:1, reactions : reactions + species] = cool_ref[...].reshape(1, species)
    cool_col[...] = jnp.broadcast_to(rows[:, reactions : reactions + LANES].T[0:padded, 0:1], cool_col.shape)

    def gather(x, found):
        order_ref[found] = x
        return found + flag_ref[x]

    live = lax.fori_loop(0, row_count, gather, jnp.int32(0))
    order_ref[live] = row_count

    for copy in small:
        copy.wait()
    for start in range(0, reactions, LANES):
        size = min(LANES, reactions - start)
        turned = rows[:, start : start + LANES].T[0:size]
        high, low = split2(tall[start : start + size, :])
        none = jnp.zeros((size, LANES - species), BF16)
        spare = lane_index((size, LANES)) >= padded
        high = jnp.concatenate([high, none], axis=1)
        ka_ref[start : start + size, 0:LANES] = jnp.where(spare, turned.astype(BF16), high)
        ka_ref[start : start + size, LANES : 2 * LANES] = jnp.concatenate([low, none], axis=1)
    none = jnp.zeros((padded - species, reactions), BF16)
    high, low = [jnp.concatenate([part, none], axis=0) for part in split2(wide[...])]
    ms_ref[0:padded] = high[:, 0:full]
    ms_ref[padded : 2 * padded] = low[:, 0:full]
    mr_ref[...] = jnp.concatenate([high[:, full:], low[:, full:], high[:, full:]], axis=1)
    largest = jnp.max(jnp.max(peaks[...], axis=0, keepdims=True), axis=1, keepdims=True)
    half_ref[...] = jnp.broadcast_to(0.5 * (COURANT / largest), half_ref.shape)
    flat_out = o_ref.reshape(row_count * species, LANES)

    def put(x, value):
        first = (x // CHUNK) * (CHUNK * species) + jnp.bitwise_and(x, CHUNK - 1)
        flat_out[pl.ds(first, species, stride=CHUNK), :] = value[0:species]

    def send(i, _):
        pltpu.make_async_copy(o_ref.at[i], out_hbm.at[:, pl.ds(i * CHUNK, CHUNK)], out_sem).start()
        return 0

    def quiet_rows(i, _):
        for copy in chunk_in(i):
            copy.wait()
        for r in range(CHUNK):
            x = i * CHUNK + r
            value = c_ref[x] + half_ref[...] * s_ref[x]
            c_ref[x, 0:species] = value[0:species]
            flat_out[pl.ds(i * (CHUNK * species) + r, species, stride=CHUNK), :] = value[0:species]
            heat_ref[pl.ds(x, 1), :] = c_ref[x, padded - 1 : padded]
        return 0

    lax.fori_loop(0, chunks, quiet_rows, 0)

    ceiling = RATE_CEILING * LOG2E

    def production(state, log_ref, high_ref, low_ref, rest_ref):
        high, low = split2(jnp.log2(jnp.abs(state) + LOG_OFFSET))
        log_ref[0:padded] = high
        log_ref[LANES : LANES + padded] = high
        log_ref[2 * LANES : 2 * LANES + padded] = low
        log_ref[3 * LANES : 3 * LANES + padded] = low
        for start in range(0, reactions, SPAN):
            stop = min(start + SPAN, reactions)
            table = ka_ref[start:stop]
            rate = mxu(table, log_ref[0 : 2 * LANES]) + mxu(table, log_ref[2 * LANES : 4 * LANES])
            high, low = split2(jnp.exp2(jnp.minimum(rate, ceiling)))
            inner = min(stop, full)
            high_ref[start:inner] = high[0 : inner - start]
            low_ref[start:inner] = low[0 : inner - start]
            if stop == reactions:
                rest_ref[...] = jnp.concatenate([high[full - start :], high[full - start :], low[full - start :]], axis=0)
        both = mxu(ms_ref[...], high_ref[...])
        return (both[0:padded] + both[padded:]) + mxu(ms_ref[0:padded], low_ref[...]) + mxu(mr_ref[...], rest_ref[...])

    def begin(places, base_ref, k_ref, sum_ref, log_ref, *_):
        for i, x in enumerate(places):
            base_ref[:, i * LANES : (i + 1) * LANES] = c_ref[x]
        heat = base_ref[padded - 1 : padded]
        parts = split3(-1.0 / heat)
        one = jnp.ones_like(parts[0])
        zero = jnp.zeros_like(one)
        extra = [one, one, one] + [parts[i] for i in (0, 1, 2, 0, 1, 0)] + [zero] * 7
        log_ref[padded:LANES] = jnp.concatenate(extra, axis=0)

    def section(index, base_ref, k_ref, sum_ref, *rest):
        if index == 0:
            k_ref[...] = production(base_ref[...], *rest)
            sum_ref[...] = k_ref[...]
        elif index < 3:
            k_ref[...] = production(base_ref[...] + 0.5 * CHEM_STEP * k_ref[...], *rest)
            sum_ref[...] += 2.0 * k_ref[...]
        else:
            sum_ref[...] += production(base_ref[...] + CHEM_STEP * k_ref[...], *rest)

    def finish(places, base_ref, k_ref, sum_ref, *_):
        result = base_ref[...] + CHEM_STEP / 6.0 * sum_ref[...]
        moved = result - base_ref[...]
        for i, x in enumerate(places):
            lanes = slice(i * LANES, (i + 1) * LANES)
            put(x, result[:, lanes])
            drop = jnp.sum(cool_col[...] * moved[:, lanes], axis=0, keepdims=True)
            heat_ref[pl.ds(x, 1), :] = base_ref[padded - 1 : padded, lanes] - drop

    def reach(count):
        return jnp.minimum(order_ref[jnp.minimum(count, live)] // CHUNK, chunks)

    sent = order_ref[0] // CHUNK
    lax.fori_loop(0, sent, send, 0)

    @pl.loop(0, (live + together - 1) // together, init_carry=sent)
    def sent(group, sent):
        first = group * together
        places = [
            [order_ref[jnp.minimum(first + n * GROUP + i, live - 1)] for i in range(GROUP)] for n in range(STREAMS)
        ]
        for rows, stream in zip(places, streams):
            begin(rows, *stream)
        for index in range(4):
            for stream in streams:
                section(index, *stream)
        for rows, stream in zip(places, streams):
            finish(rows, *stream)
        done = order_ref[jnp.minimum(first + together, live)] // CHUNK
        lax.fori_loop(sent, done, send, 0)
        return done

    lax.fori_loop(sent, chunks, send, 0)

    heat_out = pltpu.make_async_copy(heat_ref, heat_hbm, heat_sem)
    heat_out.start()

    def wait_out(i, _):
        pltpu.make_async_copy(o_ref.at[0], out_hbm.at[:, pl.ds(0, CHUNK)], out_sem).wait()
        return 0

    lax.fori_loop(0, chunks, wait_out, 0)
    heat_out.wait()


def per_device(levels, heat, inverse, factor, exponents, energies, change, cooling, flags):
    row_count, species, _ = levels.shape
    reactions = factor.shape[0]
    padded = -(-species // 16) * 16
    across = -(-reactions // LANES) * LANES + LANES
    chunks = row_count // CHUNK
    full = reactions // LANES * LANES
    rest = reactions - full
    devices = 1
    for axis in FLOW_CHEM:
        devices *= lax.axis_size(axis)
    far = pl.BlockSpec(memory_space=pltpu.HBM)

    def shape(*dims, dtype=F32):
        return jax.ShapeDtypeStruct(dims, dtype)

    plane = (row_count, padded, LANES)
    def side():
        return pltpu.VMEM((padded, LANES), F32)

    cells, spread, mine_even, mine_odd, cols, peak = pl.pallas_call(
        functools.partial(spread_kernel, species),
        in_specs=[far, far, far],
        out_specs=[far] * 6,
        out_shape=[
            shape(*plane), shape(*plane),
            shape(padded, LANES), shape(padded, LANES), shape(padded, LANES), shape(devices, LANES),
        ],
        scratch_shapes=[
            side(), pltpu.VMEM((devices, LANES), F32),
            pltpu.VMEM((chunks, species, CHUNK, LANES), F32), pltpu.VMEM(plane, F32), pltpu.VMEM(plane, F32),
            pltpu.VMEM((row_count, LANES), F32), pltpu.VMEM((species, species), F32),
            pltpu.VMEM((2 * padded, padded), BF16), side(), side(),
            pltpu.SemaphoreType.DMA((chunks,)), pltpu.SemaphoreType.DMA((2,)), pltpu.SemaphoreType.DMA((4,)),
            pltpu.SemaphoreType.DMA,
        ],
        cost_estimate=pl.CostEstimate(flops=10**9, bytes_accessed=11 * 10**6, transcendentals=0),
        name="spread",
    )(levels.transpose(1, 0, 2), heat, inverse)

    def swap(value, axis, first):
        pairs = []
        for i in range(first, lax.axis_size(axis) - 1, 2):
            pairs += [(i, i + 1), (i + 1, i)]
        return lax.ppermute(value, axis, pairs)

    peaks = lax.all_to_all(peak, FLOW_CHEM, 0, 0, tiled=True)
    even = swap(mine_even, FLOW, 0)
    odd = swap(mine_odd, FLOW, 1)
    pair = swap(cols, "chem", 0)
    cross = swap(cols, "chem", 1)

    fluxes = pl.pallas_call(
        flux_kernel,
        in_specs=[far] * 8,
        out_specs=far,
        out_shape=shape(*plane),
        scratch_shapes=[
            pltpu.VMEM((row_count + 1, padded, LANES), F32), pltpu.VMEM((row_count + 1, padded, LANES), F32),
            pltpu.VMEM(plane, F32), pltpu.VMEM((5, padded, LANES), F32), pltpu.VMEM((species, species), F32),
            pltpu.VMEM((2 * padded, padded), BF16), side(), side(), side(),
            pltpu.VMEM((2, 2 * LANES, 2 * LANES), BF16),
            pltpu.SemaphoreType.DMA((2, chunks)), pltpu.SemaphoreType.DMA((6,)), pltpu.SemaphoreType.DMA,
        ],
        cost_estimate=pl.CostEstimate(flops=10**9, bytes_accessed=11 * 10**6, transcendentals=0),
        name="flux",
    )(cells, spread, even, odd, pair, cross, cols, inverse)

    span = GROUP * LANES
    out, heat_out = pl.pallas_call(
        functools.partial(advance_kernel, species, reactions),
        in_specs=[far] * 9,
        out_specs=[far, far],
        out_shape=[shape(species, row_count, LANES), shape(row_count, LANES)],
        scratch_shapes=[
            pltpu.SMEM((row_count,), jnp.int32), pltpu.VMEM((reactions,), F32), pltpu.VMEM((reactions,), F32),
            pltpu.VMEM((species,), F32), pltpu.VMEM((row_count, LANES), F32),
            pltpu.VMEM(plane, F32), pltpu.VMEM(plane, F32), pltpu.VMEM((chunks, species, CHUNK, LANES), F32),
            pltpu.SMEM((row_count + 1,), jnp.int32), side(),
            pltpu.VMEM((devices, LANES), F32),
            pltpu.VMEM((LANES, across), F32), pltpu.VMEM((reactions, species), F32),
            pltpu.VMEM((species, reactions), F32), pltpu.VMEM((reactions, 2 * LANES), BF16),
            pltpu.VMEM((2 * padded, full), BF16), pltpu.VMEM((padded, 3 * rest), BF16),
            side(), pltpu.SemaphoreType.DMA((3,)),
            pltpu.SemaphoreType.DMA((4,)), pltpu.SemaphoreType.DMA,
        ]
        + STREAMS * [
            pltpu.VMEM((padded, span), F32), pltpu.VMEM((padded, span), F32), pltpu.VMEM((padded, span), F32),
            pltpu.VMEM((4 * LANES, span), BF16),
            pltpu.VMEM((full, span), BF16), pltpu.VMEM((full, span), BF16), pltpu.VMEM((3 * rest, span), BF16),
        ]
        + [
            pltpu.SemaphoreType.DMA((2, chunks)), pltpu.SemaphoreType.DMA,
        ],
        cost_estimate=pl.CostEstimate(flops=2 * 10**10, bytes_accessed=11 * 10**6, transcendentals=0),
        name="advance",
    )(
        flags.reshape(-1), peaks, cells, fluxes, factor, exponents, energies, change, cooling,
    )
    return out.transpose(1, 0, 2), heat_out


def solution(mesh):
    torus = Mesh(
        mesh.devices.reshape(4, 4, 2, mesh.shape["chem"]), ("flow_0", "flow_1", "flow_2", "chem")
    )
    placed = (P(FLOW, None, "chem"), P(FLOW, "chem"), P(), P(), P(), P(), P(), P(), P(FLOW, "chem"))
    return jax.shard_map(
        per_device,
        mesh=torus,
        in_specs=placed,
        out_specs=(P(FLOW, None, "chem"), P(FLOW, "chem")),
        check_vma=False,
    )
```

```python
import functools

import jax
import jax.numpy as jnp
from jax import lax
from jax.experimental import pallas as pl
from jax.experimental.pallas import tpu as pltpu
from jax.sharding import Mesh
from jax.sharding import PartitionSpec as P

FLOW = ("flow_0", "flow_1", "flow_2")
FLOW_CHEM = ("flow_0", "flow_1", "flow_2", "chem")

COURANT = 0.2
CHEM_STEP = 0.05
LOG_OFFSET = 0.001
RATE_CEILING = 2.0
LOG2E = 1.4426950408889634

F32 = jnp.float32
BF16 = jnp.bfloat16
LANES = 128
GROUP = 4
STREAMS = 2
SPAN = 784
CHUNK = 8
HALF = 16


def split2(value):
    high = value.astype(BF16)
    return high, (value - high.astype(F32)).astype(BF16)


def split3(value):
    high = value.astype(BF16)
    rest = value - high.astype(F32)
    mid = rest.astype(BF16)
    return high, mid, (rest - mid.astype(F32)).astype(BF16)


def mxu(lhs, rhs):
    return jnp.dot(lhs, rhs, preferred_element_type=F32)


def mixture(cells, stacked):
    padded = cells.shape[0]
    high, low = split2(cells)
    both = mxu(stacked[...], high)
    total = both[:padded] + both[padded:] + mxu(stacked[0:padded], low)
    heat = cells[padded - 1 : padded]
    there = heat > 0.0
    scaled = heat * jnp.sqrt(heat)
    return jnp.where(there, scaled, 0.0) / jnp.where(there, total, 1.0)


def lane_index(shape):
    return lax.broadcasted_iota(jnp.int32, shape, len(shape) - 1)


def stack_inverse(stacked, inverse):
    species = inverse.shape[0]
    padded = stacked.shape[0] // 2
    none = jnp.zeros((species, padded - species), BF16)
    for first, part in zip((0, padded), split2(inverse[...])):
        part = jnp.concatenate([part, none], axis=1)
        stacked[first : first + padded] = jnp.concatenate([part, part[0 : padded - species]], axis=0)


def spread_kernel(
    species,
    x_hbm, t_hbm, r_hbm,
    c_hbm, d_hbm, even_hbm, odd_hbm, cols_hbm, peak_hbm,
    cols_ref, peak_ref, x_buf, c_buf, d_buf, heat, square, rs_ref, first_col, last_col, in_sems, small_sems, end_sems, out_sem,
):
    row_count, padded, _ = c_buf.shape
    chunks = row_count // CHUNK

    def chunk_in(i):
        return pltpu.make_async_copy(x_hbm.at[:, pl.ds(i * CHUNK, CHUNK)], x_buf.at[i], in_sems.at[i])

    chunk_in(0).start()
    heat_in = pltpu.make_async_copy(t_hbm, heat, small_sems.at[0])
    heat_in.start()
    inverse_in = pltpu.make_async_copy(r_hbm, square, small_sems.at[1])
    inverse_in.start()
    for i in range(1, chunks):
        chunk_in(i).start()

    first_col[...] = jnp.zeros_like(first_col)
    last_col[...] = jnp.zeros_like(last_col)
    lane = lane_index((padded, LANES))
    inverse_in.wait()
    stack_inverse(rs_ref, square)
    heat_in.wait()

    def send(buf, hbm, i):
        here = pl.ds(i * CHUNK, CHUNK)
        pltpu.make_async_copy(buf.at[here], hbm.at[here], out_sem).start()

    def chunk(i, peak):
        chunk_in(i).wait()
        flat = x_buf.at[i].reshape(species * CHUNK, LANES)
        base = i * CHUNK
        first = jnp.zeros((padded, LANES), F32)
        last = jnp.zeros((padded, LANES), F32)
        for pair in range(0, CHUNK, 2):
            x = base + pair
            for r in (pair, pair + 1):
                c_buf[base + r, 0:species] = flat[pl.ds(r, species, stride=CHUNK), :]
                c_buf[base + r, species:padded] = heat[pl.ds(base + r, 1), :]
            row = [c_buf[x], c_buf[x + 1]]
            high, low = split2(jnp.concatenate(row, axis=1))
            both = mxu(rs_ref[...], high)
            total = both[:padded] + both[padded:] + mxu(rs_ref[0:padded], low)
            warm = jnp.concatenate([heat[pl.ds(x, 1), :], heat[pl.ds(x + 1, 1), :]], axis=1)
            spread = warm * jnp.sqrt(warm) / total
            thin = [spread[:, 0:LANES], spread[:, LANES:]]
            peak = jnp.maximum(peak, jnp.maximum(thin[0], thin[1]))

            d_buf[x] = thin[0]
            d_buf[x + 1] = thin[1]
            for r, value in zip((pair, pair + 1), row):
                value = pltpu.roll(value, r, 1) if r else value
                first = jnp.where(lane == r, value, first)
                last = jnp.where(lane == (r - 1) % LANES, value, last)
        here = lane // CHUNK == i
        first_col[...] = jnp.where(here, pltpu.roll(first, base, 1), first_col[...])
        last_col[...] = jnp.where(here, pltpu.roll(last, base + 1, 1), last_col[...])
        send(c_buf, c_hbm, i)
        send(d_buf, d_hbm, i)
        return peak

    peak = lax.fori_loop(0, chunks, chunk, jnp.zeros((padded, LANES), F32))
    best = jnp.max(jnp.max(peak, axis=0, keepdims=True), axis=1, keepdims=True)
    peak_ref[...] = jnp.broadcast_to(best, peak_ref.shape)
    cols_ref[...] = jnp.where(lane < 64, first_col[...], pltpu.roll(last_col[...], 64, 1))
    flipped = lax.axis_index(FLOW[-1]) * (row_count - 1)
    ends = [
        pltpu.make_async_copy(src, dst, end_sems.at[n])
        for n, (src, dst) in enumerate((
            (peak_ref, peak_hbm), (cols_ref, cols_hbm),
            (c_buf.at[row_count - 1 - flipped], even_hbm), (c_buf.at[flipped], odd_hbm),
        ))
    ]
    for copy in ends:
        copy.start()
    for copy in ends:
        copy.wait()
    pltpu.make_async_copy(c_buf, c_hbm, out_sem).wait()
    pltpu.make_async_copy(d_buf, d_hbm, out_sem).wait()


def flux_kernel(
    c_hbm, d_hbm, even_hbm, odd_hbm, pair_hbm, cross_hbm, cols_hbm, r_hbm, s_hbm,
    c_ref, d_ref, s_ref, sides, square, rs_ref, first_ref, last_ref, gap_ref, step_ref, in_sems, small_sems, out_sem,
):
    row_count, padded, _ = s_ref.shape
    chunks = row_count // CHUNK
    lane = lane_index((padded, LANES))

    def chunk_in(i):
        here = pl.ds(i * CHUNK, CHUNK)
        return (
            pltpu.make_async_copy(c_hbm.at[here], c_ref.at[here], in_sems.at[0, i]),
            pltpu.make_async_copy(d_hbm.at[here], d_ref.at[here], in_sems.at[1, i]),
        )

    small = [pltpu.make_async_copy(r_hbm, square, small_sems.at[0])]
    for n, side in enumerate((even_hbm, odd_hbm, pair_hbm, cross_hbm, cols_hbm)):
        small.append(pltpu.make_async_copy(side, sides.at[n], small_sems.at[n + 1]))
    for copy in small:
        copy.start()
    for i in range(chunks):
        for copy in chunk_in(i):
            copy.start()

    rows = jnp.bitwise_and(lax.broadcasted_iota(jnp.int32, (2 * LANES, 2 * LANES), 0), LANES - 1)
    cell = lane_index((2 * LANES, 2 * LANES))
    back = cell >= LANES
    cell = jnp.bitwise_and(cell, LANES - 1)
    beside = jnp.where(back, cell - 1, cell + 1)
    inside = jnp.logical_and(beside >= 0, beside < LANES)
    there = jnp.where(jnp.logical_and(inside, rows == beside), 1.0, 0.0)
    here = jnp.where(jnp.logical_and(inside, rows == cell), 1.0, 0.0)
    step_ref[0] = (there - here).astype(BF16)
    step_ref[1] = (there + here).astype(BF16)
    for copy in small:
        copy.wait()
    stack_inverse(rs_ref, square)

    odd = lax.axis_index(FLOW[-1]) == 1
    above = jnp.where(odd, sides[0], sides[1])
    below = jnp.where(odd, sides[1], sides[0])
    odd = lax.rem(lax.axis_index("chem"), 2) == 1
    left = jnp.where(odd, sides[2], sides[3])
    right = jnp.where(odd, sides[3], sides[2])
    beyond = pltpu.roll(jnp.where(lane < 64, right, left), 64, 1)
    mine = sides[4]
    spread = mixture(jnp.concatenate([mine, beyond], axis=1), rs_ref)
    edge = (spread[:, 0:LANES] + spread[:, LANES:]) * (beyond - mine)
    first_ref[...] = edge
    last_ref[...] = pltpu.roll(edge, 63, 1)
    outer = mixture(jnp.concatenate([above, below], axis=1), rs_ref)
    c_ref[row_count] = below
    d_ref[row_count] = outer[:, LANES:]

    def wait_in(i):
        for copy in chunk_in(i):
            copy.wait()

    def beside_of(ref, base, which):
        value = ref[pl.ds(base, HALF)].reshape(HALF * padded, LANES)
        return mxu(jnp.concatenate(split2(value), axis=1), step_ref[which])

    for i in range(HALF // CHUNK):
        wait_in(i)
    gap_ref[...] = (d_ref[0] + outer[:, 0:LANES]) * (c_ref[0] - above)

    @pl.loop(0, row_count // HALF)
    def _(part):
        base = part * HALF

        @pl.when(part < row_count // HALF - 1)
        def _():
            for n in range(HALF // CHUNK):
                wait_in((part + 1) * (HALF // CHUNK) + n)

        change = beside_of(c_ref, base, 0)
        total = beside_of(d_ref, base, 1)
        along = change * total
        along = along[:, 0:LANES] + along[:, LANES:]
        gap = gap_ref[...]
        for r in range(HALF):
            x = base + r
            later = (d_ref[x] + d_ref[x + 1]) * (c_ref[x + 1] - c_ref[x])
            ends = pltpu.roll(jnp.where(lane == x, first_ref[...], last_ref[...]), LANES - x, 1)
            ends = jnp.where(jnp.logical_or(lane == 0, lane == LANES - 1), ends, 0.0)
            s_ref[x] = (along[r * padded : (r + 1) * padded] + ends) + (later - gap)
            gap = later
        gap_ref[...] = gap

        done = pl.ds(base, HALF)
        pltpu.make_async_copy(s_ref.at[done], s_hbm.at[done], out_sem).start()

    pltpu.make_async_copy(s_ref, s_hbm, out_sem).wait()


def advance_kernel(
    species, reactions,
    flag_hbm, peak_hbm, c_hbm, s_hbm, a_hbm, k_hbm, e_hbm, m_hbm, cool_hbm,
    out_hbm, heat_hbm,
    flag_ref, a_ref, e_ref, cool_ref, heat_ref, c_ref, s_ref, o_ref, order_ref, half_ref, peaks, rows, tall, wide,
    ka_ref, ms_ref, mr_ref, cool_col, small_sems, early_sems, heat_sem, *rest,
):
    streams = [rest[i * 7 : i * 7 + 7] for i in range(STREAMS)]
    in_sems, out_sem = rest[STREAMS * 7 :]
    row_count, padded, _ = c_ref.shape
    full = ms_ref.shape[1]
    chunks = row_count // CHUNK
    together = STREAMS * GROUP

    def chunk_in(i):
        here = pl.ds(i * CHUNK, CHUNK)
        return (
            pltpu.make_async_copy(c_hbm.at[here], c_ref.at[here], in_sems.at[0, i]),
            pltpu.make_async_copy(s_hbm.at[here], s_ref.at[here], in_sems.at[1, i]),
        )

    small = [
        pltpu.make_async_copy(*ends, small_sems.at[n])
        for n, ends in enumerate(
            ((peak_hbm, peaks), (k_hbm, tall), (m_hbm, wide))
        )
    ]
    early = [
        pltpu.make_async_copy(*ends, early_sems.at[n])
        for n, ends in enumerate(((flag_hbm, flag_ref), (a_hbm, a_ref), (e_hbm, e_ref), (cool_hbm, cool_ref)))
    ]
    for copy in early:
        copy.start()
    for copy in small:
        copy.start()
    for i in range(chunks):
        for copy in chunk_in(i):
            copy.start()

    rows[...] = jnp.zeros_like(rows)
    for stream in streams:
        stream[3][...] = jnp.zeros_like(stream[3])
    for copy in early:
        copy.wait()
    factors = split3(a_ref[...].reshape(1, reactions) * LOG2E)
    energies = split3(e_ref[...].reshape(1, reactions) * LOG2E)
    order = [factors[0], factors[1], factors[2]] + [energies[i] for i in (0, 0, 0, 1, 1, 2)]
    for i, row in enumerate(order):
        rows[padded + i : padded + i + 1, 0:reactions] = row.astype(F32)
    rows[0:1, reactions : reactions + species] = cool_ref[...].reshape(1, species)
    cool_col[...] = jnp.broadcast_to(rows[:, reactions : reactions + LANES].T[0:padded, 0:1], cool_col.shape)

    def gather(x, found):
        order_ref[found] = x
        return found + flag_ref[x]

    live = lax.fori_loop(0, row_count, gather, jnp.int32(0), unroll=16)
    order_ref[live] = row_count

    for copy in small:
        copy.wait()
    for start in range(0, reactions, LANES):
        size = min(LANES, reactions - start)
        turned = rows[:, start : start + LANES].T[0:size]
        high, low = split2(tall[start : start + size, :])
        none = jnp.zeros((size, LANES - species), BF16)
        spare = lane_index((size, LANES)) >= padded
        high = jnp.concatenate([high, none], axis=1)
        ka_ref[start : start + size, 0:LANES] = jnp.where(spare, turned.astype(BF16), high)
        ka_ref[start : start + size, LANES : 2 * LANES] = jnp.concatenate([low, none], axis=1)
    none = jnp.zeros((padded - species, reactions), BF16)
    high, low = [jnp.concatenate([part, none], axis=0) for part in split2(wide[...])]
    ms_ref[0:padded] = high[:, 0:full]
    ms_ref[padded : 2 * padded] = low[:, 0:full]
    mr_ref[...] = jnp.concatenate([high[:, full:], low[:, full:], high[:, full:]], axis=1)
    largest = jnp.max(jnp.max(peaks[...], axis=0, keepdims=True), axis=1, keepdims=True)
    half_ref[...] = jnp.broadcast_to(0.5 * (COURANT / largest), half_ref.shape)
    flat_out = o_ref.reshape(row_count * species, LANES)

    def put(x, value):
        first = (x // CHUNK) * (CHUNK * species) + jnp.bitwise_and(x, CHUNK - 1)
        flat_out[pl.ds(first, species, stride=CHUNK), :] = value[0:species]

    def send(i, _):
        pltpu.make_async_copy(o_ref.at[i], out_hbm.at[:, pl.ds(i * CHUNK, CHUNK)], out_sem).start()
        return 0

    def quiet_rows(i, _):
        for copy in chunk_in(i):
            copy.wait()
        for r in range(CHUNK):
            x = i * CHUNK + r
            value = c_ref[x] + half_ref[...] * s_ref[x]
            c_ref[x, 0:species] = value[0:species]
            flat_out[pl.ds(i * (CHUNK * species) + r, species, stride=CHUNK), :] = value[0:species]
            heat_ref[pl.ds(x, 1), :] = c_ref[x, padded - 1 : padded]
        return 0

    lax.fori_loop(0, chunks, quiet_rows, 0)

    ceiling = RATE_CEILING * LOG2E

    def production(state, log_ref, high_ref, low_ref, rest_ref):
        high, low = split2(jnp.log2(jnp.abs(state) + LOG_OFFSET))
        log_ref[0:padded] = high
        log_ref[LANES : LANES + padded] = high
        log_ref[2 * LANES : 2 * LANES + padded] = low
        log_ref[3 * LANES : 3 * LANES + padded] = low
        for start in range(0, reactions, SPAN):
            stop = min(start + SPAN, reactions)
            table = ka_ref[start:stop]
            rate = mxu(table, log_ref[0 : 2 * LANES]) + mxu(table, log_ref[2 * LANES : 4 * LANES])
            high, low = split2(jnp.exp2(jnp.minimum(rate, ceiling)))
            inner = min(stop, full)
            high_ref[start:inner] = high[0 : inner - start]
            low_ref[start:inner] = low[0 : inner - start]
            if stop == reactions:
                rest_ref[...] = jnp.concatenate([high[full - start :], high[full - start :], low[full - start :]], axis=0)
        both = mxu(ms_ref[...], high_ref[...])
        return (both[0:padded] + both[padded:]) + mxu(ms_ref[0:padded], low_ref[...]) + mxu(mr_ref[...], rest_ref[...])

    def begin(places, base_ref, k_ref, sum_ref, log_ref, *_):
        for i, x in enumerate(places):
            base_ref[:, i * LANES : (i + 1) * LANES] = c_ref[x]
        heat = base_ref[padded - 1 : padded]
        parts = split3(-1.0 / heat)
        one = jnp.ones_like(parts[0])
        zero = jnp.zeros_like(one)
        extra = [one, one, one] + [parts[i] for i in (0, 1, 2, 0, 1, 0)] + [zero] * 7
        log_ref[padded:LANES] = jnp.concatenate(extra, axis=0)

    def section(index, base_ref, k_ref, sum_ref, *rest):
        if index == 0:
            k_ref[...] = production(base_ref[...], *rest)
            sum_ref[...] = k_ref[...]
        elif index < 3:
            k_ref[...] = production(base_ref[...] + 0.5 * CHEM_STEP * k_ref[...], *rest)
            sum_ref[...] += 2.0 * k_ref[...]
        else:
            sum_ref[...] += production(base_ref[...] + CHEM_STEP * k_ref[...], *rest)

    def finish(places, base_ref, k_ref, sum_ref, *_):
        result = base_ref[...] + CHEM_STEP / 6.0 * sum_ref[...]
        moved = result - base_ref[...]
        for i, x in enumerate(places):
            lanes = slice(i * LANES, (i + 1) * LANES)
            put(x, result[:, lanes])
            drop = jnp.sum(cool_col[...] * moved[:, lanes], axis=0, keepdims=True)
            heat_ref[pl.ds(x, 1), :] = base_ref[padded - 1 : padded, lanes] - drop

    def reach(count):
        return jnp.minimum(order_ref[jnp.minimum(count, live)] // CHUNK, chunks)

    sent = order_ref[0] // CHUNK
    lax.fori_loop(0, sent, send, 0)

    @pl.loop(0, (live + together - 1) // together, init_carry=sent)
    def sent(group, sent):
        first = group * together
        places = [
            [order_ref[jnp.minimum(first + n * GROUP + i, live - 1)] for i in range(GROUP)] for n in range(STREAMS)
        ]
        for rows, stream in zip(places, streams):
            begin(rows, *stream)
        for index in range(4):
            for stream in streams:
                section(index, *stream)
        for rows, stream in zip(places, streams):
            finish(rows, *stream)
        done = order_ref[jnp.minimum(first + together, live)] // CHUNK
        lax.fori_loop(sent, done, send, 0)
        return done

    lax.fori_loop(sent, chunks, send, 0)

    heat_out = pltpu.make_async_copy(heat_ref, heat_hbm, heat_sem)
    heat_out.start()

    def wait_out(i, _):
        pltpu.make_async_copy(o_ref.at[0], out_hbm.at[:, pl.ds(0, CHUNK)], out_sem).wait()
        return 0

    lax.fori_loop(0, chunks, wait_out, 0)
    heat_out.wait()


def per_device(levels, heat, inverse, factor, exponents, energies, change, cooling, flags):
    row_count, species, _ = levels.shape
    reactions = factor.shape[0]
    padded = -(-species // 16) * 16
    across = -(-reactions // LANES) * LANES + LANES
    chunks = row_count // CHUNK
    full = reactions // LANES * LANES
    rest = reactions - full
    devices = 1
    for axis in FLOW_CHEM:
        devices *= lax.axis_size(axis)
    far = pl.BlockSpec(memory_space=pltpu.HBM)

    def shape(*dims, dtype=F32):
        return jax.ShapeDtypeStruct(dims, dtype)

    plane = (row_count, padded, LANES)
    def side():
        return pltpu.VMEM((padded, LANES), F32)

    cells, spread, mine_even, mine_odd, cols, peak = pl.pallas_call(
        functools.partial(spread_kernel, species),
        in_specs=[far, far, far],
        out_specs=[far] * 6,
        out_shape=[
            shape(*plane), shape(*plane),
            shape(padded, LANES), shape(padded, LANES), shape(padded, LANES), shape(devices, LANES),
        ],
        scratch_shapes=[
            side(), pltpu.VMEM((devices, LANES), F32),
            pltpu.VMEM((chunks, species, CHUNK, LANES), F32), pltpu.VMEM(plane, F32), pltpu.VMEM(plane, F32),
            pltpu.VMEM((row_count, LANES), F32), pltpu.VMEM((species, species), F32),
            pltpu.VMEM((2 * padded, padded), BF16), side(), side(),
            pltpu.SemaphoreType.DMA((chunks,)), pltpu.SemaphoreType.DMA((2,)), pltpu.SemaphoreType.DMA((4,)),
            pltpu.SemaphoreType.DMA,
        ],
        cost_estimate=pl.CostEstimate(flops=10**9, bytes_accessed=11 * 10**6, transcendentals=0),
        name="spread",
    )(levels.transpose(1, 0, 2), heat, inverse)

    def swap(value, axis, first):
        pairs = []
        for i in range(first, lax.axis_size(axis) - 1, 2):
            pairs += [(i, i + 1), (i + 1, i)]
        return lax.ppermute(value, axis, pairs)

    peaks = lax.all_to_all(peak, FLOW_CHEM, 0, 0, tiled=True)
    even = swap(mine_even, FLOW, 0)
    odd = swap(mine_odd, FLOW, 1)
    pair = swap(cols, "chem", 0)
    cross = swap(cols, "chem", 1)

    fluxes = pl.pallas_call(
        flux_kernel,
        in_specs=[far] * 8,
        out_specs=far,
        out_shape=shape(*plane),
        scratch_shapes=[
            pltpu.VMEM((row_count + 1, padded, LANES), F32), pltpu.VMEM((row_count + 1, padded, LANES), F32),
            pltpu.VMEM(plane, F32), pltpu.VMEM((5, padded, LANES), F32), pltpu.VMEM((species, species), F32),
            pltpu.VMEM((2 * padded, padded), BF16), side(), side(), side(),
            pltpu.VMEM((2, 2 * LANES, 2 * LANES), BF16),
            pltpu.SemaphoreType.DMA((2, chunks)), pltpu.SemaphoreType.DMA((6,)), pltpu.SemaphoreType.DMA,
        ],
        cost_estimate=pl.CostEstimate(flops=10**9, bytes_accessed=11 * 10**6, transcendentals=0),
        name="flux",
    )(cells, spread, even, odd, pair, cross, cols, inverse)

    span = GROUP * LANES
    out, heat_out = pl.pallas_call(
        functools.partial(advance_kernel, species, reactions),
        in_specs=[far] * 9,
        out_specs=[far, far],
        out_shape=[shape(species, row_count, LANES), shape(row_count, LANES)],
        scratch_shapes=[
            pltpu.SMEM((row_count,), jnp.int32), pltpu.VMEM((reactions,), F32), pltpu.VMEM((reactions,), F32),
            pltpu.VMEM((species,), F32), pltpu.VMEM((row_count, LANES), F32),
            pltpu.VMEM(plane, F32), pltpu.VMEM(plane, F32), pltpu.VMEM((chunks, species, CHUNK, LANES), F32),
            pltpu.SMEM((row_count + 1,), jnp.int32), side(),
            pltpu.VMEM((devices, LANES), F32),
            pltpu.VMEM((LANES, across), F32), pltpu.VMEM((reactions, species), F32),
            pltpu.VMEM((species, reactions), F32), pltpu.VMEM((reactions, 2 * LANES), BF16),
            pltpu.VMEM((2 * padded, full), BF16), pltpu.VMEM((padded, 3 * rest), BF16),
            side(), pltpu.SemaphoreType.DMA((3,)),
            pltpu.SemaphoreType.DMA((4,)), pltpu.SemaphoreType.DMA,
        ]
        + STREAMS * [
            pltpu.VMEM((padded, span), F32), pltpu.VMEM((padded, span), F32), pltpu.VMEM((padded, span), F32),
            pltpu.VMEM((4 * LANES, span), BF16),
            pltpu.VMEM((full, span), BF16), pltpu.VMEM((full, span), BF16), pltpu.VMEM((3 * rest, span), BF16),
        ]
        + [
            pltpu.SemaphoreType.DMA((2, chunks)), pltpu.SemaphoreType.DMA,
        ],
        cost_estimate=pl.CostEstimate(flops=2 * 10**10, bytes_accessed=11 * 10**6, transcendentals=0),
        name="advance",
    )(
        flags.reshape(-1), peaks, cells, fluxes, factor, exponents, energies, change, cooling,
    )
    return out.transpose(1, 0, 2), heat_out


def solution(mesh):
    torus = Mesh(
        mesh.devices.reshape(4, 4, 2, mesh.shape["chem"]), ("flow_0", "flow_1", "flow_2", "chem")
    )
    placed = (P(FLOW, None, "chem"), P(FLOW, "chem"), P(), P(), P(), P(), P(), P(), P(FLOW, "chem"))
    return jax.shard_map(
        per_device,
        mesh=torus,
        in_specs=placed,
        out_specs=(P(FLOW, None, "chem"), P(FLOW, "chem")),
        check_vma=False,
    )
```

```python
import functools

import jax
import jax.numpy as jnp
from jax import lax
from jax.experimental import pallas as pl
from jax.experimental.pallas import tpu as pltpu
from jax.sharding import Mesh
from jax.sharding import PartitionSpec as P

FLOW = ("flow_0", "flow_1", "flow_2")
FLOW_CHEM = ("flow_0", "flow_1", "flow_2", "chem")

COURANT = 0.2
CHEM_STEP = 0.05
LOG_OFFSET = 0.001
RATE_CEILING = 2.0
LOG2E = 1.4426950408889634

F32 = jnp.float32
BF16 = jnp.bfloat16
LANES = 128
GROUP = 4
STREAMS = 2
SPAN = 784
CHUNK = 8
TOGETHER = 2
HALF = 16


def split2(value):
    high = value.astype(BF16)
    return high, (value - high.astype(F32)).astype(BF16)


def split3(value):
    high = value.astype(BF16)
    rest = value - high.astype(F32)
    mid = rest.astype(BF16)
    return high, mid, (rest - mid.astype(F32)).astype(BF16)


def mxu(lhs, rhs):
    return jnp.dot(lhs, rhs, preferred_element_type=F32)


def mixture(cells, stacked):
    padded = cells.shape[0]
    high, low = split2(cells)
    both = mxu(stacked[...], high)
    total = both[:padded] + both[padded:] + mxu(stacked[0:padded], low)
    heat = cells[padded - 1 : padded]
    there = heat > 0.0
    scaled = heat * jnp.sqrt(heat)
    return jnp.where(there, scaled, 0.0) / jnp.where(there, total, 1.0)


def lane_index(shape):
    return lax.broadcasted_iota(jnp.int32, shape, len(shape) - 1)


def stack_inverse(stacked, inverse):
    species = inverse.shape[0]
    padded = stacked.shape[0] // 2
    none = jnp.zeros((species, padded - species), BF16)
    for first, part in zip((0, padded), split2(inverse[...])):
        part = jnp.concatenate([part, none], axis=1)
        stacked[first : first + padded] = jnp.concatenate([part, part[0 : padded - species]], axis=0)


def spread_kernel(
    species,
    x_hbm, t_hbm, r_hbm,
    c_hbm, d_hbm, even_hbm, odd_hbm, cols_hbm, peak_hbm,
    cols_ref, peak_ref, x_buf, c_buf, d_buf, heat, square, rs_ref, first_col, last_col, in_sems, small_sems, end_sems, out_sem,
):
    row_count, padded, _ = c_buf.shape
    chunks = row_count // CHUNK

    def chunk_in(i):
        return pltpu.make_async_copy(x_hbm.at[:, pl.ds(i * CHUNK, CHUNK)], x_buf.at[i], in_sems.at[i])

    chunk_in(0).start()
    heat_in = pltpu.make_async_copy(t_hbm, heat, small_sems.at[0])
    heat_in.start()
    inverse_in = pltpu.make_async_copy(r_hbm, square, small_sems.at[1])
    inverse_in.start()
    for i in range(1, chunks):
        chunk_in(i).start()

    first_col[...] = jnp.zeros_like(first_col)
    last_col[...] = jnp.zeros_like(last_col)
    lane = lane_index((padded, LANES))
    inverse_in.wait()
    stack_inverse(rs_ref, square)
    heat_in.wait()

    def some(step, peak):
        for n in range(TOGETHER):
            chunk_in(step * TOGETHER + n).wait()
        for n in range(TOGETHER):
            peak = chunk(step * TOGETHER + n, peak)
        rows = pl.ds(step * (TOGETHER * CHUNK), TOGETHER * CHUNK)
        pltpu.make_async_copy(c_buf.at[rows], c_hbm.at[rows], out_sem).start()
        pltpu.make_async_copy(d_buf.at[rows], d_hbm.at[rows], out_sem).start()
        return peak

    def chunk(i, peak):
        flat = x_buf.at[i].reshape(species * CHUNK, LANES)
        base = i * CHUNK
        first = jnp.zeros((padded, LANES), F32)
        last = jnp.zeros((padded, LANES), F32)
        for pair in range(0, CHUNK, 2):
            x = base + pair
            for r in (pair, pair + 1):
                c_buf[base + r, 0:species] = flat[pl.ds(r, species, stride=CHUNK), :]
                c_buf[base + r, species:padded] = heat[pl.ds(base + r, 1), :]
            row = [c_buf[x], c_buf[x + 1]]
            high, low = split2(jnp.concatenate(row, axis=1))
            both = mxu(rs_ref[...], high)
            total = both[:padded] + both[padded:] + mxu(rs_ref[0:padded], low)
            warm = jnp.concatenate([heat[pl.ds(x, 1), :], heat[pl.ds(x + 1, 1), :]], axis=1)
            spread = warm * jnp.sqrt(warm) / total
            thin = [spread[:, 0:LANES], spread[:, LANES:]]
            peak = jnp.maximum(peak, jnp.maximum(thin[0], thin[1]))

            d_buf[x] = thin[0]
            d_buf[x + 1] = thin[1]
            for r, value in zip((pair, pair + 1), row):
                value = pltpu.roll(value, r, 1) if r else value
                first = jnp.where(lane == r, value, first)
                last = jnp.where(lane == (r - 1) % LANES, value, last)
        here = lane // CHUNK == i
        first_col[...] = jnp.where(here, pltpu.roll(first, base, 1), first_col[...])
        last_col[...] = jnp.where(here, pltpu.roll(last, base + 1, 1), last_col[...])
        return peak

    peak = lax.fori_loop(0, chunks // TOGETHER, some, jnp.zeros((padded, LANES), F32))
    best = jnp.max(jnp.max(peak, axis=0, keepdims=True), axis=1, keepdims=True)
    peak_ref[...] = jnp.broadcast_to(best, peak_ref.shape)
    cols_ref[...] = jnp.where(lane < 64, first_col[...], pltpu.roll(last_col[...], 64, 1))
    flipped = lax.axis_index(FLOW[-1]) * (row_count - 1)
    ends = [
        pltpu.make_async_copy(src, dst, end_sems.at[n])
        for n, (src, dst) in enumerate((
            (peak_ref, peak_hbm), (cols_ref, cols_hbm),
            (c_buf.at[row_count - 1 - flipped], even_hbm), (c_buf.at[flipped], odd_hbm),
        ))
    ]
    for copy in ends:
        copy.start()
    for copy in ends:
        copy.wait()
    pltpu.make_async_copy(c_buf, c_hbm, out_sem).wait()
    pltpu.make_async_copy(d_buf, d_hbm, out_sem).wait()


def flux_kernel(
    c_hbm, d_hbm, even_hbm, odd_hbm, pair_hbm, cross_hbm, cols_hbm, r_hbm, s_hbm,
    c_ref, d_ref, s_ref, sides, square, rs_ref, first_ref, last_ref, gap_ref, step_ref, in_sems, small_sems, out_sem,
):
    row_count, padded, _ = s_ref.shape
    chunks = row_count // CHUNK
    lane = lane_index((padded, LANES))

    def chunk_in(i):
        here = pl.ds(i * CHUNK, CHUNK)
        return (
            pltpu.make_async_copy(c_hbm.at[here], c_ref.at[here], in_sems.at[0, i]),
            pltpu.make_async_copy(d_hbm.at[here], d_ref.at[here], in_sems.at[1, i]),
        )

    small = [pltpu.make_async_copy(r_hbm, square, small_sems.at[0])]
    for n, side in enumerate((even_hbm, odd_hbm, pair_hbm, cross_hbm, cols_hbm)):
        small.append(pltpu.make_async_copy(side, sides.at[n], small_sems.at[n + 1]))
    for copy in small:
        copy.start()
    for i in range(chunks):
        for copy in chunk_in(i):
            copy.start()

    rows = jnp.bitwise_and(lax.broadcasted_iota(jnp.int32, (2 * LANES, 2 * LANES), 0), LANES - 1)
    cell = lane_index((2 * LANES, 2 * LANES))
    back = cell >= LANES
    cell = jnp.bitwise_and(cell, LANES - 1)
    beside = jnp.where(back, cell - 1, cell + 1)
    inside = jnp.logical_and(beside >= 0, beside < LANES)
    there = jnp.where(jnp.logical_and(inside, rows == beside), 1.0, 0.0)
    here = jnp.where(jnp.logical_and(inside, rows == cell), 1.0, 0.0)
    step_ref[0] = (there - here).astype(BF16)
    step_ref[1] = (there + here).astype(BF16)
    for copy in small:
        copy.wait()
    stack_inverse(rs_ref, square)

    odd = lax.axis_index(FLOW[-1]) == 1
    above = jnp.where(odd, sides[0], sides[1])
    below = jnp.where(odd, sides[1], sides[0])
    odd = lax.rem(lax.axis_index("chem"), 2) == 1
    left = jnp.where(odd, sides[2], sides[3])
    right = jnp.where(odd, sides[3], sides[2])
    beyond = pltpu.roll(jnp.where(lane < 64, right, left), 64, 1)
    mine = sides[4]
    spread = mixture(jnp.concatenate([mine, beyond], axis=1), rs_ref)
    edge = (spread[:, 0:LANES] + spread[:, LANES:]) * (beyond - mine)
    first_ref[...] = edge
    last_ref[...] = pltpu.roll(edge, 63, 1)
    outer = mixture(jnp.concatenate([above, below], axis=1), rs_ref)
    c_ref[row_count] = below
    d_ref[row_count] = outer[:, LANES:]

    def wait_in(i):
        for copy in chunk_in(i):
            copy.wait()

    def beside_of(ref, base, which):
        value = ref[pl.ds(base, HALF)].reshape(HALF * padded, LANES)
        return mxu(jnp.concatenate(split2(value), axis=1), step_ref[which])

    for i in range(HALF // CHUNK):
        wait_in(i)
    gap_ref[...] = (d_ref[0] + outer[:, 0:LANES]) * (c_ref[0] - above)

    @pl.loop(0, row_count // HALF)
    def _(part):
        base = part * HALF

        @pl.when(part < row_count // HALF - 1)
        def _():
            for n in range(HALF // CHUNK):
                wait_in((part + 1) * (HALF // CHUNK) + n)

        change = beside_of(c_ref, base, 0)
        total = beside_of(d_ref, base, 1)
        along = change * total
        along = along[:, 0:LANES] + along[:, LANES:]
        gap = gap_ref[...]
        for r in range(HALF):
            x = base + r
            later = (d_ref[x] + d_ref[x + 1]) * (c_ref[x + 1] - c_ref[x])
            ends = pltpu.roll(jnp.where(lane == x, first_ref[...], last_ref[...]), LANES - x, 1)
            ends = jnp.where(jnp.logical_or(lane == 0, lane == LANES - 1), ends, 0.0)
            s_ref[x] = (along[r * padded : (r + 1) * padded] + ends) + (later - gap)
            gap = later
        gap_ref[...] = gap

        done = pl.ds(base, HALF)
        pltpu.make_async_copy(s_ref.at[done], s_hbm.at[done], out_sem).start()

    pltpu.make_async_copy(s_ref, s_hbm, out_sem).wait()


def advance_kernel(
    species, reactions,
    flag_hbm, peak_hbm, c_hbm, s_hbm, a_hbm, k_hbm, e_hbm, m_hbm, cool_hbm,
    out_hbm, heat_hbm,
    flag_ref, a_ref, e_ref, cool_ref, heat_ref, c_ref, s_ref, o_ref, order_ref, half_ref, peaks, rows, tall, wide,
    ka_ref, ms_ref, mr_ref, cool_col, small_sems, early_sems, heat_sem, *rest,
):
    streams = [rest[i * 7 : i * 7 + 7] for i in range(STREAMS)]
    in_sems, out_sem = rest[STREAMS * 7 :]
    row_count, padded, _ = c_ref.shape
    full = ms_ref.shape[1]
    chunks = row_count // CHUNK
    together = STREAMS * GROUP

    def chunk_in(i):
        here = pl.ds(i * CHUNK, CHUNK)
        return (
            pltpu.make_async_copy(c_hbm.at[here], c_ref.at[here], in_sems.at[0, i]),
            pltpu.make_async_copy(s_hbm.at[here], s_ref.at[here], in_sems.at[1, i]),
        )

    small = [
        pltpu.make_async_copy(*ends, small_sems.at[n])
        for n, ends in enumerate(
            ((peak_hbm, peaks), (k_hbm, tall), (m_hbm, wide))
        )
    ]
    early = [
        pltpu.make_async_copy(*ends, early_sems.at[n])
        for n, ends in enumerate(((flag_hbm, flag_ref), (a_hbm, a_ref), (e_hbm, e_ref), (cool_hbm, cool_ref)))
    ]
    for copy in early:
        copy.start()
    for copy in small:
        copy.start()
    for i in range(chunks):
        for copy in chunk_in(i):
            copy.start()

    rows[...] = jnp.zeros_like(rows)
    for stream in streams:
        stream[3][...] = jnp.zeros_like(stream[3])
    for copy in early:
        copy.wait()
    factors = split3(a_ref[...].reshape(1, reactions) * LOG2E)
    energies = split3(e_ref[...].reshape(1, reactions) * LOG2E)
    order = [factors[0], factors[1], factors[2]] + [energies[i] for i in (0, 0, 0, 1, 1, 2)]
    for i, row in enumerate(order):
        rows[padded + i : padded + i + 1, 0:reactions] = row.astype(F32)
    rows[0:1, reactions : reactions + species] = cool_ref[...].reshape(1, species)
    cool_col[...] = jnp.broadcast_to(rows[:, reactions : reactions + LANES].T[0:padded, 0:1], cool_col.shape)

    def gather(x, found):
        order_ref[found] = x
        return found + flag_ref[x]

    live = lax.fori_loop(0, row_count, gather, jnp.int32(0), unroll=16)
    order_ref[live] = row_count

    for copy in small:
        copy.wait()
    for start in range(0, reactions, LANES):
        size = min(LANES, reactions - start)
        turned = rows[:, start : start + LANES].T[0:size]
        high, low = split2(tall[start : start + size, :])
        none = jnp.zeros((size, LANES - species), BF16)
        spare = lane_index((size, LANES)) >= padded
        high = jnp.concatenate([high, none], axis=1)
        ka_ref[start : start + size, 0:LANES] = jnp.where(spare, turned.astype(BF16), high)
        ka_ref[start : start + size, LANES : 2 * LANES] = jnp.concatenate([low, none], axis=1)
    none = jnp.zeros((padded - species, reactions), BF16)
    high, low = [jnp.concatenate([part, none], axis=0) for part in split2(wide[...])]
    ms_ref[0:padded] = high[:, 0:full]
    ms_ref[padded : 2 * padded] = low[:, 0:full]
    mr_ref[...] = jnp.concatenate([high[:, full:], low[:, full:], high[:, full:]], axis=1)
    largest = jnp.max(jnp.max(peaks[...], axis=0, keepdims=True), axis=1, keepdims=True)
    half_ref[...] = jnp.broadcast_to(0.5 * (COURANT / largest), half_ref.shape)
    flat_out = o_ref.reshape(row_count * species, LANES)

    def put(x, value):
        first = (x // CHUNK) * (CHUNK * species) + jnp.bitwise_and(x, CHUNK - 1)
        flat_out[pl.ds(first, species, stride=CHUNK), :] = value[0:species]

    def send(i, _):
        pltpu.make_async_copy(o_ref.at[i], out_hbm.at[:, pl.ds(i * CHUNK, CHUNK)], out_sem).start()
        return 0

    def quiet_pair(step, _):
        for n in (0, 1):
            for copy in chunk_in(2 * step + n):
                copy.wait()
        quiet_rows(2 * step)
        quiet_rows(2 * step + 1)
        return 0

    def quiet_rows(i):
        for r in range(CHUNK):
            x = i * CHUNK + r
            value = c_ref[x] + half_ref[...] * s_ref[x]
            c_ref[x, 0:species] = value[0:species]
            flat_out[pl.ds(i * (CHUNK * species) + r, species, stride=CHUNK), :] = value[0:species]
            heat_ref[pl.ds(x, 1), :] = c_ref[x, padded - 1 : padded]

    lax.fori_loop(0, chunks // 2, quiet_pair, 0)

    ceiling = RATE_CEILING * LOG2E

    def production(state, log_ref, high_ref, low_ref, rest_ref):
        high, low = split2(jnp.log2(jnp.abs(state) + LOG_OFFSET))
        log_ref[0:padded] = high
        log_ref[LANES : LANES + padded] = high
        log_ref[2 * LANES : 2 * LANES + padded] = low
        log_ref[3 * LANES : 3 * LANES + padded] = low
        for start in range(0, reactions, SPAN):
            stop = min(start + SPAN, reactions)
            table = ka_ref[start:stop]
            rate = mxu(table, log_ref[0 : 2 * LANES]) + mxu(table, log_ref[2 * LANES : 4 * LANES])
            high, low = split2(jnp.exp2(jnp.minimum(rate, ceiling)))
            inner = min(stop, full)
            high_ref[start:inner] = high[0 : inner - start]
            low_ref[start:inner] = low[0 : inner - start]
            if stop == reactions:
                rest_ref[...] = jnp.concatenate([high[full - start :], high[full - start :], low[full - start :]], axis=0)
        both = mxu(ms_ref[...], high_ref[...])
        return (both[0:padded] + both[padded:]) + mxu(ms_ref[0:padded], low_ref[...]) + mxu(mr_ref[...], rest_ref[...])

    def begin(places, base_ref, k_ref, sum_ref, log_ref, *_):
        for i, x in enumerate(places):
            base_ref[:, i * LANES : (i + 1) * LANES] = c_ref[x]
        heat = base_ref[padded - 1 : padded]
        parts = split3(-1.0 / heat)
        one = jnp.ones_like(parts[0])
        zero = jnp.zeros_like(one)
        extra = [one, one, one] + [parts[i] for i in (0, 1, 2, 0, 1, 0)] + [zero] * 7
        log_ref[padded:LANES] = jnp.concatenate(extra, axis=0)

    def section(index, base_ref, k_ref, sum_ref, *rest):
        if index == 0:
            k_ref[...] = production(base_ref[...], *rest)
            sum_ref[...] = k_ref[...]
        elif index < 3:
            k_ref[...] = production(base_ref[...] + 0.5 * CHEM_STEP * k_ref[...], *rest)
            sum_ref[...] += 2.0 * k_ref[...]
        else:
            sum_ref[...] += production(base_ref[...] + CHEM_STEP * k_ref[...], *rest)

    def finish(places, base_ref, k_ref, sum_ref, *_):
        result = base_ref[...] + CHEM_STEP / 6.0 * sum_ref[...]
        moved = result - base_ref[...]
        for i, x in enumerate(places):
            lanes = slice(i * LANES, (i + 1) * LANES)
            put(x, result[:, lanes])
            drop = jnp.sum(cool_col[...] * moved[:, lanes], axis=0, keepdims=True)
            heat_ref[pl.ds(x, 1), :] = base_ref[padded - 1 : padded, lanes] - drop

    def reach(count):
        return jnp.minimum(order_ref[jnp.minimum(count, live)] // CHUNK, chunks)

    sent = order_ref[0] // CHUNK
    lax.fori_loop(0, sent, send, 0)

    @pl.loop(0, (live + together - 1) // together, init_carry=sent)
    def sent(group, sent):
        first = group * together
        places = [
            [order_ref[jnp.minimum(first + n * GROUP + i, live - 1)] for i in range(GROUP)] for n in range(STREAMS)
        ]
        for rows, stream in zip(places, streams):
            begin(rows, *stream)
        for index in range(4):
            for stream in streams:
                section(index, *stream)
        for rows, stream in zip(places, streams):
            finish(rows, *stream)
        done = order_ref[jnp.minimum(first + together, live)] // CHUNK
        lax.fori_loop(sent, done, send, 0)
        return done

    lax.fori_loop(sent, chunks, send, 0)

    heat_out = pltpu.make_async_copy(heat_ref, heat_hbm, heat_sem)
    heat_out.start()

    def wait_out(i, _):
        pltpu.make_async_copy(o_ref.at[0], out_hbm.at[:, pl.ds(0, CHUNK)], out_sem).wait()
        return 0

    lax.fori_loop(0, chunks, wait_out, 0)
    heat_out.wait()


def per_device(levels, heat, inverse, factor, exponents, energies, change, cooling, flags):
    row_count, species, _ = levels.shape
    reactions = factor.shape[0]
    padded = -(-species // 16) * 16
    across = -(-reactions // LANES) * LANES + LANES
    chunks = row_count // CHUNK
    full = reactions // LANES * LANES
    rest = reactions - full
    devices = 1
    for axis in FLOW_CHEM:
        devices *= lax.axis_size(axis)
    far = pl.BlockSpec(memory_space=pltpu.HBM)

    def shape(*dims, dtype=F32):
        return jax.ShapeDtypeStruct(dims, dtype)

    plane = (row_count, padded, LANES)
    def side():
        return pltpu.VMEM((padded, LANES), F32)

    cells, spread, mine_even, mine_odd, cols, peak = pl.pallas_call(
        functools.partial(spread_kernel, species),
        in_specs=[far, far, far],
        out_specs=[far] * 6,
        out_shape=[
            shape(*plane), shape(*plane),
            shape(padded, LANES), shape(padded, LANES), shape(padded, LANES), shape(devices, LANES),
        ],
        scratch_shapes=[
            side(), pltpu.VMEM((devices, LANES), F32),
            pltpu.VMEM((chunks, species, CHUNK, LANES), F32), pltpu.VMEM(plane, F32), pltpu.VMEM(plane, F32),
            pltpu.VMEM((row_count, LANES), F32), pltpu.VMEM((species, species), F32),
            pltpu.VMEM((2 * padded, padded), BF16), side(), side(),
            pltpu.SemaphoreType.DMA((chunks,)), pltpu.SemaphoreType.DMA((2,)), pltpu.SemaphoreType.DMA((4,)),
            pltpu.SemaphoreType.DMA,
        ],
        cost_estimate=pl.CostEstimate(flops=10**9, bytes_accessed=11 * 10**6, transcendentals=0),
        name="spread",
    )(levels.transpose(1, 0, 2), heat, inverse)

    def swap(value, axis, first):
        pairs = []
        for i in range(first, lax.axis_size(axis) - 1, 2):
            pairs += [(i, i + 1), (i + 1, i)]
        return lax.ppermute(value, axis, pairs)

    peaks = lax.all_to_all(peak, FLOW_CHEM, 0, 0, tiled=True)
    even = swap(mine_even, FLOW, 0)
    odd = swap(mine_odd, FLOW, 1)
    pair = swap(cols, "chem", 0)
    cross = swap(cols, "chem", 1)

    fluxes = pl.pallas_call(
        flux_kernel,
        in_specs=[far] * 8,
        out_specs=far,
        out_shape=shape(*plane),
        scratch_shapes=[
            pltpu.VMEM((row_count + 1, padded, LANES), F32), pltpu.VMEM((row_count + 1, padded, LANES), F32),
            pltpu.VMEM(plane, F32), pltpu.VMEM((5, padded, LANES), F32), pltpu.VMEM((species, species), F32),
            pltpu.VMEM((2 * padded, padded), BF16), side(), side(), side(),
            pltpu.VMEM((2, 2 * LANES, 2 * LANES), BF16),
            pltpu.SemaphoreType.DMA((2, chunks)), pltpu.SemaphoreType.DMA((6,)), pltpu.SemaphoreType.DMA,
        ],
        cost_estimate=pl.CostEstimate(flops=10**9, bytes_accessed=11 * 10**6, transcendentals=0),
        name="flux",
    )(cells, spread, even, odd, pair, cross, cols, inverse)

    span = GROUP * LANES
    out, heat_out = pl.pallas_call(
        functools.partial(advance_kernel, species, reactions),
        in_specs=[far] * 9,
        out_specs=[far, far],
        out_shape=[shape(species, row_count, LANES), shape(row_count, LANES)],
        scratch_shapes=[
            pltpu.SMEM((row_count,), jnp.int32), pltpu.VMEM((reactions,), F32), pltpu.VMEM((reactions,), F32),
            pltpu.VMEM((species,), F32), pltpu.VMEM((row_count, LANES), F32),
            pltpu.VMEM(plane, F32), pltpu.VMEM(plane, F32), pltpu.VMEM((chunks, species, CHUNK, LANES), F32),
            pltpu.SMEM((row_count + 1,), jnp.int32), side(),
            pltpu.VMEM((devices, LANES), F32),
            pltpu.VMEM((LANES, across), F32), pltpu.VMEM((reactions, species), F32),
            pltpu.VMEM((species, reactions), F32), pltpu.VMEM((reactions, 2 * LANES), BF16),
            pltpu.VMEM((2 * padded, full), BF16), pltpu.VMEM((padded, 3 * rest), BF16),
            side(), pltpu.SemaphoreType.DMA((3,)),
            pltpu.SemaphoreType.DMA((4,)), pltpu.SemaphoreType.DMA,
        ]
        + STREAMS * [
            pltpu.VMEM((padded, span), F32), pltpu.VMEM((padded, span), F32), pltpu.VMEM((padded, span), F32),
            pltpu.VMEM((4 * LANES, span), BF16),
            pltpu.VMEM((full, span), BF16), pltpu.VMEM((full, span), BF16), pltpu.VMEM((3 * rest, span), BF16),
        ]
        + [
            pltpu.SemaphoreType.DMA((2, chunks)), pltpu.SemaphoreType.DMA,
        ],
        cost_estimate=pl.CostEstimate(flops=2 * 10**10, bytes_accessed=11 * 10**6, transcendentals=0),
        name="advance",
    )(
        flags.reshape(-1), peaks, cells, fluxes, factor, exponents, energies, change, cooling,
    )
    return out.transpose(1, 0, 2), heat_out


def solution(mesh):
    torus = Mesh(
        mesh.devices.reshape(4, 4, 2, mesh.shape["chem"]), ("flow_0", "flow_1", "flow_2", "chem")
    )
    placed = (P(FLOW, None, "chem"), P(FLOW, "chem"), P(), P(), P(), P(), P(), P(), P(FLOW, "chem"))
    return jax.shard_map(
        per_device,
        mesh=torus,
        in_specs=placed,
        out_specs=(P(FLOW, None, "chem"), P(FLOW, "chem")),
        check_vma=False,
    )
```

```python
import functools

import jax
import jax.numpy as jnp
from jax import lax
from jax.experimental import pallas as pl
from jax.experimental.pallas import tpu as pltpu
from jax.sharding import Mesh
from jax.sharding import PartitionSpec as P

FLOW = ("flow_0", "flow_1", "flow_2")
FLOW_CHEM = ("flow_0", "flow_1", "flow_2", "chem")

COURANT = 0.2
CHEM_STEP = 0.05
LOG_OFFSET = 0.001
RATE_CEILING = 2.0
LOG2E = 1.4426950408889634

F32 = jnp.float32
BF16 = jnp.bfloat16
LANES = 128
GROUP = 4
STREAMS = 2
SPAN = 784
CHUNK = 8
TOGETHER = 2
HALF = 16


def split2(value):
    high = value.astype(BF16)
    return high, (value - high.astype(F32)).astype(BF16)


def split3(value):
    high = value.astype(BF16)
    rest = value - high.astype(F32)
    mid = rest.astype(BF16)
    return high, mid, (rest - mid.astype(F32)).astype(BF16)


def mxu(lhs, rhs):
    return jnp.dot(lhs, rhs, preferred_element_type=F32)


def mixture(cells, stacked):
    padded = cells.shape[0]
    high, low = split2(cells)
    both = mxu(stacked[...], high)
    total = both[:padded] + both[padded:] + mxu(stacked[0:padded], low)
    heat = cells[padded - 1 : padded]
    there = heat > 0.0
    scaled = heat * jnp.sqrt(heat)
    return jnp.where(there, scaled, 0.0) / jnp.where(there, total, 1.0)


def lane_index(shape):
    return lax.broadcasted_iota(jnp.int32, shape, len(shape) - 1)


def stack_inverse(stacked, inverse):
    species = inverse.shape[0]
    padded = stacked.shape[0] // 2
    none = jnp.zeros((species, padded - species), BF16)
    for first, part in zip((0, padded), split2(inverse[...])):
        part = jnp.concatenate([part, none], axis=1)
        stacked[first : first + padded] = jnp.concatenate([part, part[0 : padded - species]], axis=0)


def spread_kernel(
    species,
    x_hbm, t_hbm, r_hbm,
    c_hbm, d_hbm, even_hbm, odd_hbm, cols_hbm, peak_hbm,
    cols_ref, peak_ref, x_buf, c_buf, d_buf, heat, square, rs_ref, first_col, last_col, in_sems, small_sems, end_sems, out_sem,
):
    row_count, padded, _ = c_buf.shape
    chunks = row_count // CHUNK

    def chunk_in(i):
        return pltpu.make_async_copy(x_hbm.at[:, pl.ds(i * CHUNK, CHUNK)], x_buf.at[i], in_sems.at[i])

    chunk_in(0).start()
    heat_in = pltpu.make_async_copy(t_hbm, heat, small_sems.at[0])
    heat_in.start()
    inverse_in = pltpu.make_async_copy(r_hbm, square, small_sems.at[1])
    inverse_in.start()
    for i in range(1, chunks):
        chunk_in(i).start()

    first_col[...] = jnp.zeros_like(first_col)
    last_col[...] = jnp.zeros_like(last_col)
    lane = lane_index((padded, LANES))
    inverse_in.wait()
    stack_inverse(rs_ref, square)
    heat_in.wait()

    def some(step, peak):
        for n in range(TOGETHER):
            chunk_in(step * TOGETHER + n).wait()
        for n in range(TOGETHER):
            peak = chunk(step * TOGETHER + n, peak)
        rows = pl.ds(step * (TOGETHER * CHUNK), TOGETHER * CHUNK)
        pltpu.make_async_copy(c_buf.at[rows], c_hbm.at[rows], out_sem).start()
        pltpu.make_async_copy(d_buf.at[rows], d_hbm.at[rows], out_sem).start()
        return peak

    def chunk(i, peak):
        flat = x_buf.at[i].reshape(species * CHUNK, LANES)
        base = i * CHUNK
        first = jnp.zeros((padded, LANES), F32)
        last = jnp.zeros((padded, LANES), F32)
        for pair in range(0, CHUNK, 2):
            x = base + pair
            for r in (pair, pair + 1):
                c_buf[base + r, 0:species] = flat[pl.ds(r, species, stride=CHUNK), :]
                c_buf[base + r, species:padded] = heat[pl.ds(base + r, 1), :]
            row = [c_buf[x], c_buf[x + 1]]
            high, low = split2(jnp.concatenate(row, axis=1))
            both = mxu(rs_ref[...], high)
            total = both[:padded] + both[padded:] + mxu(rs_ref[0:padded], low)
            warm = jnp.concatenate([heat[pl.ds(x, 1), :], heat[pl.ds(x + 1, 1), :]], axis=1)
            spread = warm * jnp.sqrt(warm) / total
            thin = [spread[:, 0:LANES], spread[:, LANES:]]
            peak = jnp.maximum(peak, jnp.maximum(thin[0], thin[1]))

            d_buf[x] = thin[0]
            d_buf[x + 1] = thin[1]
            for r, value in zip((pair, pair + 1), row):
                value = pltpu.roll(value, r, 1) if r else value
                first = jnp.where(lane == r, value, first)
                last = jnp.where(lane == (r - 1) % LANES, value, last)
        here = lane // CHUNK == i
        first_col[...] = jnp.where(here, pltpu.roll(first, base, 1), first_col[...])
        last_col[...] = jnp.where(here, pltpu.roll(last, base + 1, 1), last_col[...])
        return peak

    peak = lax.fori_loop(0, chunks // TOGETHER, some, jnp.zeros((padded, LANES), F32))
    best = jnp.max(jnp.max(peak, axis=0, keepdims=True), axis=1, keepdims=True)
    peak_ref[...] = jnp.broadcast_to(best, peak_ref.shape)
    cols_ref[...] = jnp.where(lane < 64, first_col[...], pltpu.roll(last_col[...], 64, 1))
    flipped = lax.axis_index(FLOW[-1]) * (row_count - 1)
    ends = [
        pltpu.make_async_copy(src, dst, end_sems.at[n])
        for n, (src, dst) in enumerate((
            (peak_ref, peak_hbm), (cols_ref, cols_hbm),
            (c_buf.at[row_count - 1 - flipped], even_hbm), (c_buf.at[flipped], odd_hbm),
        ))
    ]
    for copy in ends:
        copy.start()
    for copy in ends:
        copy.wait()
    pltpu.make_async_copy(c_buf, c_hbm, out_sem).wait()
    pltpu.make_async_copy(d_buf, d_hbm, out_sem).wait()


def flux_kernel(
    c_hbm, d_hbm, even_hbm, odd_hbm, pair_hbm, cross_hbm, cols_hbm, r_hbm, s_hbm,
    c_ref, d_ref, s_ref, sides, square, rs_ref, first_ref, last_ref, gap_ref, step_ref, in_sems, small_sems, out_sem,
):
    row_count, padded, _ = s_ref.shape
    chunks = row_count // CHUNK
    lane = lane_index((padded, LANES))

    def chunk_in(i):
        here = pl.ds(i * CHUNK, CHUNK)
        return (
            pltpu.make_async_copy(c_hbm.at[here], c_ref.at[here], in_sems.at[0, i]),
            pltpu.make_async_copy(d_hbm.at[here], d_ref.at[here], in_sems.at[1, i]),
        )

    small = [pltpu.make_async_copy(r_hbm, square, small_sems.at[0])]
    for n, side in enumerate((even_hbm, odd_hbm, pair_hbm, cross_hbm, cols_hbm)):
        small.append(pltpu.make_async_copy(side, sides.at[n], small_sems.at[n + 1]))
    for copy in small:
        copy.start()
    for i in range(chunks):
        for copy in chunk_in(i):
            copy.start()

    rows = jnp.bitwise_and(lax.broadcasted_iota(jnp.int32, (2 * LANES, 2 * LANES), 0), LANES - 1)
    cell = lane_index((2 * LANES, 2 * LANES))
    back = cell >= LANES
    cell = jnp.bitwise_and(cell, LANES - 1)
    beside = jnp.where(back, cell - 1, cell + 1)
    inside = jnp.logical_and(beside >= 0, beside < LANES)
    there = jnp.where(jnp.logical_and(inside, rows == beside), 1.0, 0.0)
    here = jnp.where(jnp.logical_and(inside, rows == cell), 1.0, 0.0)
    step_ref[0] = (there - here).astype(BF16)
    step_ref[1] = (there + here).astype(BF16)
    for copy in small:
        copy.wait()
    stack_inverse(rs_ref, square)

    odd = lax.axis_index(FLOW[-1]) == 1
    above = jnp.where(odd, sides[0], sides[1])
    below = jnp.where(odd, sides[1], sides[0])
    odd = lax.rem(lax.axis_index("chem"), 2) == 1
    left = jnp.where(odd, sides[2], sides[3])
    right = jnp.where(odd, sides[3], sides[2])
    beyond = pltpu.roll(jnp.where(lane < 64, right, left), 64, 1)
    mine = sides[4]
    spread = mixture(jnp.concatenate([mine, beyond], axis=1), rs_ref)
    edge = (spread[:, 0:LANES] + spread[:, LANES:]) * (beyond - mine)
    first_ref[...] = edge
    last_ref[...] = pltpu.roll(edge, 63, 1)
    outer = mixture(jnp.concatenate([above, below], axis=1), rs_ref)
    c_ref[row_count] = below
    d_ref[row_count] = outer[:, LANES:]

    def wait_in(i):
        for copy in chunk_in(i):
            copy.wait()

    def wait_chunk(i, _):
        wait_in(i)
        return 0

    def beside_of(ref, base, which):
        value = ref[pl.ds(base, HALF)].reshape(HALF * padded, LANES)
        return mxu(jnp.concatenate(split2(value), axis=1), step_ref[which])

    for i in range(HALF // CHUNK + 1):
        wait_in(i)
    gap_ref[...] = (d_ref[0] + outer[:, 0:LANES]) * (c_ref[0] - above)

    @pl.loop(0, row_count // HALF)
    def _(part):
        base = part * HALF

        ready = part * (HALF // CHUNK) + 1
        fresh = jnp.where(part == 0, ready + HALF // CHUNK, ready)
        lax.fori_loop(fresh, jnp.minimum(ready + HALF // CHUNK, chunks), wait_chunk, 0)

        change = beside_of(c_ref, base, 0)
        total = beside_of(d_ref, base, 1)
        along = change * total
        along = along[:, 0:LANES] + along[:, LANES:]
        gap = gap_ref[...]
        for r in range(HALF):
            x = base + r
            later = (d_ref[x] + d_ref[x + 1]) * (c_ref[x + 1] - c_ref[x])
            ends = pltpu.roll(jnp.where(lane == x, first_ref[...], last_ref[...]), LANES - x, 1)
            ends = jnp.where(jnp.logical_or(lane == 0, lane == LANES - 1), ends, 0.0)
            s_ref[x] = (along[r * padded : (r + 1) * padded] + ends) + (later - gap)
            gap = later
        gap_ref[...] = gap

        done = pl.ds(base, HALF)
        pltpu.make_async_copy(s_ref.at[done], s_hbm.at[done], out_sem).start()

    pltpu.make_async_copy(s_ref, s_hbm, out_sem).wait()


def advance_kernel(
    species, reactions,
    flag_hbm, peak_hbm, c_hbm, s_hbm, a_hbm, k_hbm, e_hbm, m_hbm, cool_hbm,
    out_hbm, heat_hbm,
    flag_ref, a_ref, e_ref, cool_ref, heat_ref, c_ref, s_ref, o_ref, order_ref, half_ref, peaks, rows, tall, wide,
    ka_ref, ms_ref, mr_ref, cool_col, small_sems, early_sems, heat_sem, *rest,
):
    streams = [rest[i * 7 : i * 7 + 7] for i in range(STREAMS)]
    in_sems, out_sem = rest[STREAMS * 7 :]
    row_count, padded, _ = c_ref.shape
    full = ms_ref.shape[1]
    chunks = row_count // CHUNK
    together = STREAMS * GROUP

    def chunk_in(i):
        here = pl.ds(i * CHUNK, CHUNK)
        return (
            pltpu.make_async_copy(c_hbm.at[here], c_ref.at[here], in_sems.at[0, i]),
            pltpu.make_async_copy(s_hbm.at[here], s_ref.at[here], in_sems.at[1, i]),
        )

    small = [
        pltpu.make_async_copy(*ends, small_sems.at[n])
        for n, ends in enumerate(
            ((peak_hbm, peaks), (k_hbm, tall), (m_hbm, wide))
        )
    ]
    early = [
        pltpu.make_async_copy(*ends, early_sems.at[n])
        for n, ends in enumerate(((flag_hbm, flag_ref), (a_hbm, a_ref), (e_hbm, e_ref), (cool_hbm, cool_ref)))
    ]
    for copy in early:
        copy.start()
    for copy in small:
        copy.start()
    for i in range(chunks):
        for copy in chunk_in(i):
            copy.start()

    rows[...] = jnp.zeros_like(rows)
    for stream in streams:
        stream[3][...] = jnp.zeros_like(stream[3])
    for copy in early:
        copy.wait()
    factors = split3(a_ref[...].reshape(1, reactions) * LOG2E)
    energies = split3(e_ref[...].reshape(1, reactions) * LOG2E)
    order = [factors[0], factors[1], factors[2]] + [energies[i] for i in (0, 0, 0, 1, 1, 2)]
    for i, row in enumerate(order):
        rows[padded + i : padded + i + 1, 0:reactions] = row.astype(F32)
    rows[0:1, reactions : reactions + species] = cool_ref[...].reshape(1, species)
    cool_col[...] = jnp.broadcast_to(rows[:, reactions : reactions + LANES].T[0:padded, 0:1], cool_col.shape)

    def gather(x, found):
        order_ref[found] = x
        return found + flag_ref[x]

    live = lax.fori_loop(0, row_count, gather, jnp.int32(0), unroll=16)
    order_ref[live] = row_count

    for copy in small:
        copy.wait()
    for start in range(0, reactions, LANES):
        size = min(LANES, reactions - start)
        turned = rows[:, start : start + LANES].T[0:size]
        high, low = split2(tall[start : start + size, :])
        none = jnp.zeros((size, LANES - species), BF16)
        spare = lane_index((size, LANES)) >= padded
        high = jnp.concatenate([high, none], axis=1)
        ka_ref[start : start + size, 0:LANES] = jnp.where(spare, turned.astype(BF16), high)
        ka_ref[start : start + size, LANES : 2 * LANES] = jnp.concatenate([low, none], axis=1)
    none = jnp.zeros((padded - species, reactions), BF16)
    high, low = [jnp.concatenate([part, none], axis=0) for part in split2(wide[...])]
    ms_ref[0:padded] = high[:, 0:full]
    ms_ref[padded : 2 * padded] = low[:, 0:full]
    mr_ref[...] = jnp.concatenate([high[:, full:], low[:, full:], high[:, full:]], axis=1)
    largest = jnp.max(jnp.max(peaks[...], axis=0, keepdims=True), axis=1, keepdims=True)
    half_ref[...] = jnp.broadcast_to(0.5 * (COURANT / largest), half_ref.shape)
    flat_out = o_ref.reshape(row_count * species, LANES)

    def put(x, value):
        first = (x // CHUNK) * (CHUNK * species) + jnp.bitwise_and(x, CHUNK - 1)
        flat_out[pl.ds(first, species, stride=CHUNK), :] = value[0:species]

    def send(i, _):
        pltpu.make_async_copy(o_ref.at[i], out_hbm.at[:, pl.ds(i * CHUNK, CHUNK)], out_sem).start()
        return 0

    def quiet_pair(step, _):
        for n in (0, 1):
            for copy in chunk_in(2 * step + n):
                copy.wait()
        quiet_rows(2 * step)
        quiet_rows(2 * step + 1)
        return 0

    def quiet_rows(i):
        for r in range(CHUNK):
            x = i * CHUNK + r
            value = c_ref[x] + half_ref[...] * s_ref[x]
            c_ref[x, 0:species] = value[0:species]
            flat_out[pl.ds(i * (CHUNK * species) + r, species, stride=CHUNK), :] = value[0:species]
            heat_ref[pl.ds(x, 1), :] = c_ref[x, padded - 1 : padded]

    lax.fori_loop(0, chunks // 2, quiet_pair, 0)

    ceiling = RATE_CEILING * LOG2E

    def production(state, log_ref, high_ref, low_ref, rest_ref):
        high, low = split2(jnp.log2(jnp.abs(state) + LOG_OFFSET))
        log_ref[0:padded] = high
        log_ref[LANES : LANES + padded] = high
        log_ref[2 * LANES : 2 * LANES + padded] = low
        log_ref[3 * LANES : 3 * LANES + padded] = low
        for start in range(0, reactions, SPAN):
            stop = min(start + SPAN, reactions)
            table = ka_ref[start:stop]
            rate = mxu(table, log_ref[0 : 2 * LANES]) + mxu(table, log_ref[2 * LANES : 4 * LANES])
            high, low = split2(jnp.exp2(jnp.minimum(rate, ceiling)))
            inner = min(stop, full)
            high_ref[start:inner] = high[0 : inner - start]
            low_ref[start:inner] = low[0 : inner - start]
            if stop == reactions:
                rest_ref[...] = jnp.concatenate([high[full - start :], high[full - start :], low[full - start :]], axis=0)
        both = mxu(ms_ref[...], high_ref[...])
        return (both[0:padded] + both[padded:]) + mxu(ms_ref[0:padded], low_ref[...]) + mxu(mr_ref[...], rest_ref[...])

    def begin(places, base_ref, k_ref, sum_ref, log_ref, *_):
        for i, x in enumerate(places):
            base_ref[:, i * LANES : (i + 1) * LANES] = c_ref[x]
        heat = base_ref[padded - 1 : padded]
        parts = split3(-1.0 / heat)
        one = jnp.ones_like(parts[0])
        zero = jnp.zeros_like(one)
        extra = [one, one, one] + [parts[i] for i in (0, 1, 2, 0, 1, 0)] + [zero] * 7
        log_ref[padded:LANES] = jnp.concatenate(extra, axis=0)

    def section(index, base_ref, k_ref, sum_ref, *rest):
        if index == 0:
            k_ref[...] = production(base_ref[...], *rest)
            sum_ref[...] = k_ref[...]
        elif index < 3:
            k_ref[...] = production(base_ref[...] + 0.5 * CHEM_STEP * k_ref[...], *rest)
            sum_ref[...] += 2.0 * k_ref[...]
        else:
            sum_ref[...] += production(base_ref[...] + CHEM_STEP * k_ref[...], *rest)

    def finish(places, base_ref, k_ref, sum_ref, *_):
        result = base_ref[...] + CHEM_STEP / 6.0 * sum_ref[...]
        moved = result - base_ref[...]
        for i, x in enumerate(places):
            lanes = slice(i * LANES, (i + 1) * LANES)
            put(x, result[:, lanes])
            drop = jnp.sum(cool_col[...] * moved[:, lanes], axis=0, keepdims=True)
            heat_ref[pl.ds(x, 1), :] = base_ref[padded - 1 : padded, lanes] - drop

    def reach(count):
        return jnp.minimum(order_ref[jnp.minimum(count, live)] // CHUNK, chunks)

    sent = order_ref[0] // CHUNK
    lax.fori_loop(0, sent, send, 0)

    @pl.loop(0, (live + together - 1) // together, init_carry=sent)
    def sent(group, sent):
        first = group * together
        places = [
            [order_ref[jnp.minimum(first + n * GROUP + i, live - 1)] for i in range(GROUP)] for n in range(STREAMS)
        ]
        for rows, stream in zip(places, streams):
            begin(rows, *stream)
        for index in range(4):
            for stream in streams:
                section(index, *stream)
        for rows, stream in zip(places, streams):
            finish(rows, *stream)
        done = order_ref[jnp.minimum(first + together, live)] // CHUNK
        lax.fori_loop(sent, done, send, 0)
        return done

    lax.fori_loop(sent, chunks, send, 0)

    heat_out = pltpu.make_async_copy(heat_ref, heat_hbm, heat_sem)
    heat_out.start()

    def wait_out(i, _):
        pltpu.make_async_copy(o_ref.at[0], out_hbm.at[:, pl.ds(0, CHUNK)], out_sem).wait()
        return 0

    lax.fori_loop(0, chunks, wait_out, 0)
    heat_out.wait()


def per_device(levels, heat, inverse, factor, exponents, energies, change, cooling, flags):
    row_count, species, _ = levels.shape
    reactions = factor.shape[0]
    padded = -(-species // 16) * 16
    across = -(-reactions // LANES) * LANES + LANES
    chunks = row_count // CHUNK
    full = reactions // LANES * LANES
    rest = reactions - full
    devices = 1
    for axis in FLOW_CHEM:
        devices *= lax.axis_size(axis)
    far = pl.BlockSpec(memory_space=pltpu.HBM)

    def shape(*dims, dtype=F32):
        return jax.ShapeDtypeStruct(dims, dtype)

    plane = (row_count, padded, LANES)
    def side():
        return pltpu.VMEM((padded, LANES), F32)

    cells, spread, mine_even, mine_odd, cols, peak = pl.pallas_call(
        functools.partial(spread_kernel, species),
        in_specs=[far, far, far],
        out_specs=[far] * 6,
        out_shape=[
            shape(*plane), shape(*plane),
            shape(padded, LANES), shape(padded, LANES), shape(padded, LANES), shape(devices, LANES),
        ],
        scratch_shapes=[
            side(), pltpu.VMEM((devices, LANES), F32),
            pltpu.VMEM((chunks, species, CHUNK, LANES), F32), pltpu.VMEM(plane, F32), pltpu.VMEM(plane, F32),
            pltpu.VMEM((row_count, LANES), F32), pltpu.VMEM((species, species), F32),
            pltpu.VMEM((2 * padded, padded), BF16), side(), side(),
            pltpu.SemaphoreType.DMA((chunks,)), pltpu.SemaphoreType.DMA((2,)), pltpu.SemaphoreType.DMA((4,)),
            pltpu.SemaphoreType.DMA,
        ],
        cost_estimate=pl.CostEstimate(flops=10**9, bytes_accessed=11 * 10**6, transcendentals=0),
        name="spread",
    )(levels.transpose(1, 0, 2), heat, inverse)

    def swap(value, axis, first):
        pairs = []
        for i in range(first, lax.axis_size(axis) - 1, 2):
            pairs += [(i, i + 1), (i + 1, i)]
        return lax.ppermute(value, axis, pairs)

    peaks = lax.all_to_all(peak, FLOW_CHEM, 0, 0, tiled=True)
    even = swap(mine_even, FLOW, 0)
    odd = swap(mine_odd, FLOW, 1)
    pair = swap(cols, "chem", 0)
    cross = swap(cols, "chem", 1)

    fluxes = pl.pallas_call(
        flux_kernel,
        in_specs=[far] * 8,
        out_specs=far,
        out_shape=shape(*plane),
        scratch_shapes=[
            pltpu.VMEM((row_count + 1, padded, LANES), F32), pltpu.VMEM((row_count + 1, padded, LANES), F32),
            pltpu.VMEM(plane, F32), pltpu.VMEM((5, padded, LANES), F32), pltpu.VMEM((species, species), F32),
            pltpu.VMEM((2 * padded, padded), BF16), side(), side(), side(),
            pltpu.VMEM((2, 2 * LANES, 2 * LANES), BF16),
            pltpu.SemaphoreType.DMA((2, chunks)), pltpu.SemaphoreType.DMA((6,)), pltpu.SemaphoreType.DMA,
        ],
        cost_estimate=pl.CostEstimate(flops=10**9, bytes_accessed=11 * 10**6, transcendentals=0),
        name="flux",
    )(cells, spread, even, odd, pair, cross, cols, inverse)

    span = GROUP * LANES
    out, heat_out = pl.pallas_call(
        functools.partial(advance_kernel, species, reactions),
        in_specs=[far] * 9,
        out_specs=[far, far],
        out_shape=[shape(species, row_count, LANES), shape(row_count, LANES)],
        scratch_shapes=[
            pltpu.SMEM((row_count,), jnp.int32), pltpu.VMEM((reactions,), F32), pltpu.VMEM((reactions,), F32),
            pltpu.VMEM((species,), F32), pltpu.VMEM((row_count, LANES), F32),
            pltpu.VMEM(plane, F32), pltpu.VMEM(plane, F32), pltpu.VMEM((chunks, species, CHUNK, LANES), F32),
            pltpu.SMEM((row_count + 1,), jnp.int32), side(),
            pltpu.VMEM((devices, LANES), F32),
            pltpu.VMEM((LANES, across), F32), pltpu.VMEM((reactions, species), F32),
            pltpu.VMEM((species, reactions), F32), pltpu.VMEM((reactions, 2 * LANES), BF16),
            pltpu.VMEM((2 * padded, full), BF16), pltpu.VMEM((padded, 3 * rest), BF16),
            side(), pltpu.SemaphoreType.DMA((3,)),
            pltpu.SemaphoreType.DMA((4,)), pltpu.SemaphoreType.DMA,
        ]
        + STREAMS * [
            pltpu.VMEM((padded, span), F32), pltpu.VMEM((padded, span), F32), pltpu.VMEM((padded, span), F32),
            pltpu.VMEM((4 * LANES, span), BF16),
            pltpu.VMEM((full, span), BF16), pltpu.VMEM((full, span), BF16), pltpu.VMEM((3 * rest, span), BF16),
        ]
        + [
            pltpu.SemaphoreType.DMA((2, chunks)), pltpu.SemaphoreType.DMA,
        ],
        cost_estimate=pl.CostEstimate(flops=2 * 10**10, bytes_accessed=11 * 10**6, transcendentals=0),
        name="advance",
    )(
        flags.reshape(-1), peaks, cells, fluxes, factor, exponents, energies, change, cooling,
    )
    return out.transpose(1, 0, 2), heat_out


def solution(mesh):
    torus = Mesh(
        mesh.devices.reshape(4, 4, 2, mesh.shape["chem"]), ("flow_0", "flow_1", "flow_2", "chem")
    )
    placed = (P(FLOW, None, "chem"), P(FLOW, "chem"), P(), P(), P(), P(), P(), P(), P(FLOW, "chem"))
    return jax.shard_map(
        per_device,
        mesh=torus,
        in_specs=placed,
        out_specs=(P(FLOW, None, "chem"), P(FLOW, "chem")),
        check_vma=False,
    )
```
